256 devices in a mesh: seq: 2 (over core), chan: 16 (over y, x), batch: 8 (over z).
Axes of the slice: x: 4, y: 4, z: 8, core: 2. Of those that a mesh axis runs over, the one named last changes fastest.
Arguments:
- ssm_input: bfloat16 [16384, 4096], P(('batch', 'seq'), 'chan'), parts along dimension 0, may hold values from -6 to 6
- gate_z: bfloat16 [16384, 4096], P(('batch', 'seq'), 'chan'), parts along dimension 0, may hold values from -6 to 6
- proj_forward: bfloat16 [2, 16384, 128], P(None, ('batch', 'seq')), parts along dimension 1, may hold values from -2 to 2
- proj_backward: bfloat16 [2, 16384, 128], P(None, ('batch', 'seq')), parts along dimension 1, may hold values from -2 to 2
- step_raw: float32 [2, 64, 16384], P(None, 'chan', ('batch', 'seq')), parts along dimension 2, may hold values from -3 to 3
- head_params: float32 [2, 2, 64], P(None, None, 'chan'), may hold values from -4 to 1, as said below
- skip_gain: float32 [64], P('chan'), may hold values from 0.25 to 2
- norm_gain: float32 [4096], P('chan'), may hold values from 0.5 to 1.5
- out_weight: bfloat16 [4096, 2048], P(None, 'chan'), may hold values from -0.09375 to 0.09375
Outputs:
- mixed: bfloat16 [16384, 2048], P(('batch', 'seq'), 'chan'), parts along dimension 0
The draws below stay inside these ranges and needn't reach their ends.
There are 8 independent parts, one for each index of `batch`. The reference program is written for one: setup_inputs(seed, part) draws one part's arguments, and reference() takes and returns one part's arrays. A program takes and returns all parts, laid end to end along the dimension named above; an argument that names none is the same for every part. Nothing has to cross between parts.
Inputs may be any that keep to these rules, and one draw needn't show every extreme that they name: `head_params`: index 0 of the second dimension holds positive decay rates, index 1 time-step biases.
All inputs are finite; a program needn't handle non-finite values.
Results may differ from the reference program's by a relative error of at most 0.0085.
Values may be sent and summed in bfloat16 or wider, within the bound.
A program may use at most 128 MiB of HBM per device.

```python
import math
import jax
import jax.numpy as jnp
from jax import lax

DMODEL = 2048
HEADS = 64
HEAD_DIM = 64
NSTATE = 128
SPAN = 256
TOK_DEV = 1024
INNER = 4096
SEQ_LEN = 2048


def draw_head_params(key, part):
    layers = []
    for direction in range(2):
        subkeys = jax.random.split(jax.random.fold_in(key, 11 + direction), 5)
        ranking = jax.random.permutation(subkeys[0], HEADS)
        strong_count = HEADS // 2
        strong = ranking < strong_count
        fast_rate = jnp.exp(jax.random.uniform(subkeys[1], (HEADS,), jnp.float32, math.log(0.025), math.log(0.045)))
        slow_rate = jnp.exp(jax.random.uniform(subkeys[2], (HEADS,), jnp.float32, math.log(2.4), math.log(24.0))) / SEQ_LEN
        fast_bias = jax.random.uniform(subkeys[3], (HEADS,), jnp.float32, -0.5, 0.5)
        slow_bias = jax.random.uniform(subkeys[4], (HEADS,), jnp.float32, -4.0, -3.0)
        decay_rates = jnp.where(strong, fast_rate, slow_rate)
        biases = jnp.where(strong, fast_bias, slow_bias)
        layers.append(jnp.stack([decay_rates, biases]))
    return jnp.stack(layers).astype(jnp.float32)


def draw_step_raw(key, part):
    subkeys = jax.random.split(jax.random.fold_in(key, 29), 2)
    jitter = jnp.clip(0.5 * jax.random.normal(subkeys[0], (2, HEADS, SEQ_LEN), jnp.float32), -1.5, 1.5)
    groups = SEQ_LEN // TOK_DEV
    offsets = jax.random.uniform(subkeys[1], (2, 1, groups), jnp.float32, -1.0, 1.0)
    return (jitter + jnp.repeat(offsets, TOK_DEV, axis=2)).astype(jnp.float32)


def levels(key, shape, shards, low, largest):
    factor_of, own = 1.0, jax.random.fold_in(key, 6)
    for dim, blocks in shards:
        heights = jnp.exp(jax.random.uniform(jax.random.fold_in(own, dim), (blocks,), jnp.float32, low / len(shards), largest / len(shards)))
        factor_of = factor_of * jnp.repeat(heights, shape[dim] // blocks).reshape([-1 if axis == dim else 1 for axis in range(len(shape))])
    return factor_of


def scatter_about(key, shape, width, reach, shards=(), held_as=jnp.bfloat16):
    result = jax.random.normal(key, shape, jnp.float32) * width
    if len(shards) > 0:
        result = levels(key, shape, shards, -0.22, 0.18) * result
    return jnp.clip(result, min=-reach, max=reach).astype(held_as)


def setup_inputs(seed: int = 0, part: int = 0) -> dict:
    arg_keys = jax.random.split(jax.random.key(seed), 10)
    own_keys = jax.random.split(jax.random.fold_in(arg_keys[9], part), 10)
    ssm_input = scatter_about(own_keys[0], (SEQ_LEN, INNER), 1.0, 6.0, ((0, 2), (1, 16)))
    gate_z = scatter_about(own_keys[1], (SEQ_LEN, INNER), 1.0, 6.0, ((0, 2), (1, 16)))
    proj_forward = scatter_about(own_keys[2], (2, SEQ_LEN, NSTATE), 0.3, 2.0, ((1, 2),))
    proj_backward = scatter_about(own_keys[3], (2, SEQ_LEN, NSTATE), 0.3, 2.0, ((1, 2),))
    step_raw = draw_step_raw(jax.random.fold_in(jax.random.fold_in(arg_keys[9], part), 71), part)
    head_params = draw_head_params(jax.random.fold_in(arg_keys[9], 71), part)
    skip_gain = jnp.clip(jnp.exp(math.log(2.0) - 2.0794415 * jax.random.uniform(arg_keys[6], (HEADS,), jnp.float32) ** levels(arg_keys[6], (HEADS,), ((0, 16),), -0.2, 0.2)), 0.25, 2.0)
    norm_gain = jnp.clip(0.5 + 1.0 * jax.random.uniform(arg_keys[7], (INNER,), jnp.float32) ** levels(arg_keys[7], (INNER,), ((0, 16),), -0.2, 0.2), 0.5, 1.5)
    out_weight = scatter_about(arg_keys[8], (INNER, DMODEL), INNER ** -0.5, 0.09375, ((1, 16),))
    return dict(ssm_input=ssm_input, gate_z=gate_z, proj_forward=proj_forward, proj_backward=proj_backward, step_raw=step_raw, head_params=head_params, skip_gain=skip_gain, norm_gain=norm_gain, out_weight=out_weight)


def ssd(values, b_rows, c_rows, steps, rates):
    length = values.shape[0]
    blocks = length // SPAN
    blocks_x = values.reshape(blocks, SPAN, HEADS, HEAD_DIM)
    blocks_b = b_rows.reshape(blocks, SPAN, NSTATE)
    blocks_c = c_rows.reshape(blocks, SPAN, NSTATE)
    blocks_dt = steps.reshape(HEADS, blocks, SPAN).transpose(1, 0, 2)
    lower_mask = jnp.tril(jnp.ones((SPAN, SPAN), dtype=bool))

    def advance(entering, inputs):
        block_x, block_b, block_c, block_dt = inputs
        cumlog = jnp.cumsum(-rates[:, None] * block_dt, axis=1)
        scores = jnp.dot(block_c, block_b.T, preferred_element_type=jnp.float32)
        log_gaps = cumlog[:, :, None] - cumlog[:, None, :]
        decays = jnp.where(lower_mask, jnp.exp(jnp.where(lower_mask, log_gaps, 0.0)), 0.0)
        weights = (scores[None] * decays * block_dt[:, None, :]).astype(jnp.bfloat16)
        intra_out = jnp.einsum('hts,shp->thp', weights.astype(jnp.float32), block_x.astype(jnp.float32))
        in_weights = jnp.exp(cumlog[:, -1:] - cumlog) * block_dt
        b_weighted = (block_b.astype(jnp.float32)[None] * in_weights[:, :, None]).astype(jnp.bfloat16)
        block_state = jnp.einsum('shp,hsn->hpn', block_x.astype(jnp.float32), b_weighted.astype(jnp.float32))
        inter = jnp.einsum('tn,hpn->thp', block_c.astype(jnp.float32), entering, precision=lax.Precision.HIGHEST)
        inter = inter * jnp.exp(cumlog).T[:, :, None]
        following = jnp.exp(cumlog[:, -1])[:, None, None] * entering + block_state
        return (following, intra_out + inter)
    initial = jnp.zeros((HEADS, HEAD_DIM, NSTATE), jnp.float32)
    _, outputs = lax.scan(advance, initial, (blocks_x, blocks_b, blocks_c, blocks_dt))
    return outputs.reshape(length, HEADS * HEAD_DIM)

def reference(ssm_input, gate_z, proj_forward, proj_backward, step_raw, head_params, skip_gain, norm_gain, out_weight):
    steps_fwd = jax.nn.softplus(step_raw[0] + head_params[0, 1][:, None])
    steps_bwd = jax.nn.softplus(step_raw[1] + head_params[1, 1][:, None])
    forward_out = ssd(ssm_input, proj_forward[0], proj_forward[1], steps_fwd, head_params[0, 0])
    backward_out = ssd(ssm_input[::-1], proj_backward[0][::-1], proj_backward[1][::-1], steps_bwd[:, ::-1], head_params[1, 0])[::-1]
    frames = ssm_input.shape[0]
    skipped = (ssm_input.reshape(frames, HEADS, HEAD_DIM).astype(jnp.float32) * skip_gain[:, None]).reshape(frames, INNER)
    gated = (forward_out + backward_out + skipped) * jax.nn.silu(gate_z.astype(jnp.float32))
    scale = lax.rsqrt(lax.optimization_barrier(jnp.sum(gated * gated, axis=1)) / INNER + 1.0)
    normed = (gated * scale[:, None] * norm_gain).astype(jnp.bfloat16)
    return jnp.dot(normed, out_weight, preferred_element_type=jnp.float32).astype(jnp.bfloat16)
```

```python
import jax
import jax.numpy as jnp
from jax import lax
from jax.experimental import pallas as pl
from jax.experimental.pallas import tpu as pltpu
from jax.sharding import PartitionSpec as P

MESH = pl.DeviceIdType.MESH
F32, BF16 = jnp.float32, jnp.bfloat16
SPAN = 256
HALF = 128
BLOCKS = 4
HEADS = 4
WIDE = 256
SIDE = 4
COLS = 128
NST = 128
INNER = 4096
LOG2E = 1.4426950408889634


def iota(shape, dim):
    return lax.broadcasted_iota(jnp.int32, shape, dim)


def dot(a, b):
    return jnp.dot(a, b, preferred_element_type=F32)


def dot_tt(a, b):
    return lax.dot_general(a, b, (((0,), (0,)), ((), ())), preferred_element_type=F32)


def dot_nt(a, b):
    return lax.dot_general(a, b, (((1,), (1,)), ((), ())), preferred_element_type=F32)


def split(v, parts):
    out = []
    for _ in range(parts - 1):
        high = v.astype(BF16).astype(F32)
        out.append(high)
        v = v - high
    out.append(v)
    return out


def kernel(
    x_hbm, z_hbm, pf_hbm, pb_hbm, st_hbm, hp, skip, gain_ref, w_hbm, out_ref,
    xv, zv, pfv, pbv, stv, w1, w2, a1, a2, os1, os2, or1, or2, ss1, ss2, so1, so2,
    expc, yv, sf, sb, ef, eb, payload, carry,
    in_sem, w_send, w_recv, st_send, st_recv, a_send, a_recv, s_send, s_recv,
    o_send, o_recv, t_send, t_recv,
):
    seq = lax.axis_index("seq")
    chan = lax.axis_index("chan")
    my_y, my_x = chan // SIDE, lax.rem(chan, SIDE)

    loads = []
    for i, (src, dst) in enumerate(
        ((st_hbm, stv), (x_hbm, xv), (pf_hbm, pfv), (pb_hbm, pbv), (z_hbm, zv))
    ):
        copy = pltpu.make_async_copy(src, dst, in_sem.at[i])
        copy.start()
        loads.append(copy)
    def tile(i):
        return pl.ds(pl.multiple_of(i * COLS, COLS), COLS)

    own_w1 = pltpu.make_async_copy(w_hbm.at[:, my_x], w1.at[:, :, tile(my_x)], in_sem.at[5])
    own_w2 = pltpu.make_async_copy(w_hbm.at[my_y], w2.at[:, :, tile(my_y)], in_sem.at[6])
    own_w1.start()
    own_w2.start()

    barrier = pltpu.get_barrier_semaphore()
    ys = [lax.rem(my_y + k, SIDE) for k in range(1, SIDE)]
    xs = [lax.rem(my_x + k, SIDE) for k in range(1, SIDE)]
    to_y = [{"chan": v * SIDE + my_x} for v in ys]
    to_x = [{"chan": my_y * SIDE + v} for v in xs]
    other = {"seq": 1 - seq}
    for dev in to_y + to_x + [other]:
        pl.semaphore_signal(barrier, inc=1, device_id=dev, device_id_type=MESH)
    pl.semaphore_wait(barrier, 7)

    def remote(src, dst, send, recv, dev):
        return pltpu.make_async_remote_copy(
            src_ref=src, dst_ref=dst, send_sem=send, recv_sem=recv,
            device_id=dev, device_id_type=MESH,
        )

    sends = []

    def start(*args):
        copy = remote(*args)
        copy.start()
        sends.append(copy)

    for k in range(3):
        start(w_hbm.at[:, xs[k]], w1.at[:, :, tile(my_x)], w_send.at[0, k], w_recv.at[0, my_x], to_x[k])
        start(w_hbm.at[ys[k]], w2.at[:, :, tile(my_y)], w_send.at[1, k], w_recv.at[1, my_y], to_y[k])

    loads[0].wait()
    row8 = iota((8, BLOCKS * SPAN), 0)
    bias = jnp.zeros((8, BLOCKS * SPAN), F32)
    rate = jnp.zeros((8, BLOCKS * SPAN), F32)
    for j in range(8):
        bias = jnp.where(row8 == j, hp[j // 4, 1, j % 4], bias)
        rate = jnp.where(row8 == j, hp[j // 4, 0, j % 4], rate)
    raw = jnp.concatenate([stv[0], stv[1]], axis=0) + bias
    dt_all = jnp.maximum(raw, 0.0) + jnp.log1p(jnp.exp(-jnp.abs(raw)))
    logs = split(-rate * dt_all, 3)
    stacked = jnp.concatenate(
        [part[:, b * SPAN : (b + 1) * SPAN] for b in range(BLOCKS) for part in logs], axis=0
    ).astype(BF16)
    t_of, s_of = iota((SPAN, SPAN), 0), iota((SPAN, SPAN), 1)
    after = t_of >= s_of
    up_to = dot(stacked, jnp.where(t_of <= s_of, 1.0, 0.0).astype(BF16))
    down_to = dot(stacked, jnp.where(after, 1.0, 0.0).astype(BF16))
    row = iota((8, SPAN), 0)
    is_fwd = row < HEADS

    sel_row, sel_col = iota((16, 2 * WIDE), 0), iota((16, 2 * WIDE), 1)
    spread = jnp.where((sel_row & 7) == (sel_col >> 6), 1.0, 0.0).astype(BF16)
    col_row, col_col = iota((32, 128), 0), iota((32, 128), 1)
    pick = jnp.where(((col_row & 7) == col_col) & (col_row < 24), 1.0, 0.0).astype(BF16)
    zero8 = jnp.zeros((8, SPAN), F32)

    cum2, cprime, dts, decays = [], [], [], []
    for copy in loads[1:4]:
        copy.wait()
    for b in range(BLOCKS):
        at = b * 24
        c_f = up_to[at : at + 8] + up_to[at + 8 : at + 16] + up_to[at + 16 : at + 24]
        c_b = down_to[at : at + 8] + down_to[at + 8 : at + 16] + down_to[at + 16 : at + 24]
        cum = jnp.where(is_fwd, c_f, c_b)
        end = jnp.where(is_fwd, cum[:, SPAN - 1 : SPAN], cum[:, 0:1])
        dt = dt_all[:, b * SPAN : (b + 1) * SPAN]
        e = jnp.exp(cum)
        w = jnp.exp(end - cum) * dt
        c2 = cum * LOG2E
        cum2.append(c2)
        cprime.append(c2 - jnp.log2(dt))
        dts.append(dt)
        e_cols = dot_tt(jnp.concatenate(split(e, 2), axis=0).astype(BF16), spread)
        w_cols = dot_tt(jnp.concatenate(split(w, 2), axis=0).astype(BF16), spread)
        expc[b] = e_cols
        decays.append((e_cols[SPAN - 1 : SPAN, :WIDE], e_cols[0:1, WIDE:]))
        xb = xv[b * SPAN : (b + 1) * SPAN, :].astype(F32)
        sf[b] = dot_tt(pfv[0, b * SPAN : (b + 1) * SPAN, :], (xb * w_cols[:, :WIDE]).astype(BF16))
        sb[b] = dot_tt(pbv[0, b * SPAN : (b + 1) * SPAN, :], (xb * w_cols[:, WIDE:]).astype(BF16))

    end_f = sf[0]
    for b in range(1, BLOCKS):
        end_f = decays[b][0] * end_f + sf[b]
    end_b = sb[BLOCKS - 1]
    for b in reversed(range(BLOCKS - 1)):
        end_b = decays[b][1] * end_b + sb[b]
    payload[...] = jnp.where(seq == 0, end_f, end_b)
    start(payload, carry, st_send.at[0], st_recv.at[0], other)

    lane = iota((SPAN, 128), 1)
    chan_row = iota((1, WIDE), 1) >> 6
    skip_row = jnp.zeros((1, WIDE), F32)
    for h in range(HEADS):
        skip_row = jnp.where(chan_row == h, skip[h], skip_row)
    for b in range(BLOCKS):
        rows = slice(b * SPAN, (b + 1) * SPAN)
        b_f, c_f = pfv[0, rows, :], pfv[1, rows, :]
        b_b, c_b = pbv[0, rows, :], pbv[1, rows, :]
        scores = jnp.where(after, dot_nt(c_f, b_f), dot_nt(c_b, b_b))
        cols = dot_tt(jnp.concatenate(split(cum2[b], 3) + [zero8], axis=0).astype(BF16), pick)
        dt_cols = dot_tt(jnp.concatenate(split(dts[b], 2), axis=0).astype(BF16), spread[:, WIDE:])
        xb = xv[rows, :]
        same = jnp.sum(c_b.astype(F32) * b_b.astype(F32), axis=1, keepdims=True)
        rest = xb.astype(F32) * (same * dt_cols + skip_row)
        for pair in range(2):
            halves = []
            for h in (2 * pair, 2 * pair + 1):
                gaps = jnp.where(
                    after,
                    cols[:, h : h + 1] - cprime[b][h : h + 1, :],
                    cols[:, 4 + h : 5 + h] - cprime[b][4 + h : 5 + h, :],
                )
                weights = (scores * jnp.exp2(gaps)).astype(BF16)
                halves.append(dot(weights, xb[:, pair * 128 : (pair + 1) * 128]))
            lanes = slice(pair * 128, (pair + 1) * 128)
            yv[b, :, lanes] = jnp.where(lane < 64, halves[0], halves[1]) + rest[:, lanes]

    remote(payload, carry, st_send.at[0], st_recv.at[0], other).wait_recv()
    came = carry[...]
    nothing = jnp.zeros_like(came)
    state = jnp.where(seq == 1, came, nothing)
    for b in range(BLOCKS):
        ef[b] = state.astype(BF16)
        state = decays[b][0] * state + sf[b]
    state = jnp.where(seq == 0, came, nothing)
    for b in reversed(range(BLOCKS)):
        eb[b] = state.astype(BF16)
        state = decays[b][1] * state + sb[b]

    loads[4].wait()
    gain = gain_ref[...]
    ones8 = jnp.ones((8, WIDE), BF16)
    ss1[my_y] = jnp.zeros((8, 128), F32)
    ss2[my_x] = jnp.zeros((8, 128), F32)
    for b in range(BLOCKS):
        rows = slice(b * SPAN, (b + 1) * SPAN)
        inter_f = dot(pfv[1, rows, :], ef[b]) * expc[b, :, :WIDE]
        inter_b = dot(pbv[1, rows, :], eb[b]) * expc[b, :, WIDE:]
        zb = zv[rows, :].astype(F32)
        gated = (yv[b] + inter_f + inter_b) * (zb / (1.0 + jnp.exp(-zb)))
        g = (gated * gain).astype(BF16)
        a1[my_y, b] = g[:HALF]
        a2[my_x, b] = g[HALF:]
        square = split(gated * gated, 2)
        sums = dot_nt(ones8, square[0].astype(BF16)) + dot_nt(ones8, square[1].astype(BF16))
        ss1[my_y, b : b + 1, :] = sums[0:1, :HALF]
        ss2[my_x, b : b + 1, :] = sums[0:1, HALF:]
        if b == BLOCKS - 1:
            for k in range(3):
                start(ss1.at[my_y], ss1.at[my_y], s_send.at[0, k], s_recv.at[0, my_y], to_y[k])
                start(ss2.at[my_x], ss2.at[my_x], s_send.at[1, k], s_recv.at[1, my_x], to_x[k])
        for k in range(3):
            start(a1.at[my_y, b], a1.at[my_y, b], a_send.at[0, k, b], a_recv.at[0, my_y, b], to_y[k])
            start(a2.at[my_x, b], a2.at[my_x, b], a_send.at[1, k, b], a_recv.at[1, my_x, b], to_x[k])

    own_w1.wait()
    own_w2.wait()
    for k in range(3):
        remote(w_hbm.at[:, my_x], w1.at[:, :, tile(xs[k])], w_send.at[0, k], w_recv.at[0, xs[k]], to_x[k]).wait_recv()
        remote(w_hbm.at[my_y], w2.at[:, :, tile(ys[k])], w_send.at[1, k], w_recv.at[1, ys[k]], to_y[k]).wait_recv()
    for b in range(BLOCKS):
        if b == BLOCKS - 1:
            for k in range(3):
                remote(ss1.at[ys[k]], ss1.at[ys[k]], s_send.at[0, k], s_recv.at[0, ys[k]], to_y[k]).wait_recv()
                remote(ss2.at[xs[k]], ss2.at[xs[k]], s_send.at[1, k], s_recv.at[1, xs[k]], to_x[k]).wait_recv()
            so1[my_x] = ss1[0] + ss1[1] + ss1[2] + ss1[3]
            so2[my_y] = ss2[0] + ss2[1] + ss2[2] + ss2[3]
            for k in range(3):
                start(so1.at[my_x], so1.at[my_x], t_send.at[0, k], t_recv.at[0, my_x], to_x[k])
                start(so2.at[my_y], so2.at[my_y], t_send.at[1, k], t_recv.at[1, my_y], to_y[k])
        for plan, (a, w, o, dest, src, peers, back) in enumerate(
            ((a1, w1, os1, or1, ys, xs, to_x), (a2, w2, os2, or2, xs, ys, to_y))
        ):
            mine = my_x if plan == 0 else my_y
            here = to_y if plan == 0 else to_x
            for k in range(3):
                remote(a.at[src[k], b], a.at[src[k], b], a_send.at[plan, k, b], a_recv.at[plan, src[k], b], here[k]).wait_recv()
            lhs = jnp.concatenate([a[j, b] for j in range(SIDE)], axis=1)
            product = dot(lhs, w[...].reshape(SIDE * WIDE, SIDE * COLS)).astype(BF16)
            for j in range(SIDE):
                o[b, j] = product[:, j * COLS : (j + 1) * COLS]
            for k in range(3):
                start(o.at[b, peers[k]], dest.at[mine, b], o_send.at[plan, k, b], o_recv.at[plan, mine, b], back[k])

    for plan, (so, peers, dev) in enumerate(((so1, xs, to_x), (so2, ys, to_y))):
        for k in range(3):
            remote(so.at[peers[k]], so.at[peers[k]], t_send.at[plan, k], t_recv.at[plan, peers[k]], dev[k]).wait_recv()
    scale_parts = []
    for so in (so1, so2):
        scale = lax.rsqrt((so[0] + so[1] + so[2] + so[3]) / INNER + 1.0)
        parts = split(scale, 3) + [jnp.zeros((8, 128), F32)]
        scale_parts.append(jnp.concatenate(parts, axis=0).astype(BF16))
    for b in range(BLOCKS):
        pick_b = jnp.where(((col_row & 7) == b) & (col_row < 24), 1.0, 0.0).astype(BF16)
        for plan, (o, dest, mine, peers, dev) in enumerate(
            ((os1, or1, my_x, xs, to_x), (os2, or2, my_y, ys, to_y))
        ):
            scale = dot_tt(scale_parts[plan], pick_b)
            total = o[b, mine].astype(F32)
            for k in range(3):
                remote(dest.at[peers[k], b], dest.at[peers[k], b], o_send.at[plan, k, b], o_recv.at[plan, peers[k], b], dev[k]).wait_recv()
                total = total + dest[peers[k], b].astype(F32)
            at = b * SPAN + plan * HALF
            out_ref[at : at + HALF, :] = (total * scale).astype(BF16)
    for copy in sends:
        copy.wait_send()


def body(ssm_input, gate_z, proj_forward, proj_backward, step_raw, head_params, skip_gain, norm_gain, out_weight):
    any_spec = pl.BlockSpec(memory_space=pl.ANY)
    smem = pl.BlockSpec(memory_space=pltpu.SMEM)
    vmem = pl.BlockSpec(memory_space=pltpu.VMEM)
    dma = pltpu.SemaphoreType.DMA
    rows = BLOCKS * SPAN
    return pl.pallas_call(
        kernel,
        out_shape=jax.ShapeDtypeStruct((rows, COLS), BF16),
        in_specs=[any_spec] * 5 + [smem, smem, vmem, any_spec],
        out_specs=vmem,
        scratch_shapes=[
            pltpu.VMEM((rows, WIDE), BF16),
            pltpu.VMEM((rows, WIDE), BF16),
            pltpu.VMEM((2, rows, NST), BF16),
            pltpu.VMEM((2, rows, NST), BF16),
            pltpu.VMEM((2, HEADS, rows), F32),
            pltpu.VMEM((SIDE, WIDE, SIDE * COLS), BF16),
            pltpu.VMEM((SIDE, WIDE, SIDE * COLS), BF16),
            pltpu.VMEM((SIDE, BLOCKS, HALF, WIDE), BF16),
            pltpu.VMEM((SIDE, BLOCKS, HALF, WIDE), BF16),
            pltpu.VMEM((BLOCKS, SIDE, HALF, COLS), BF16),
            pltpu.VMEM((BLOCKS, SIDE, HALF, COLS), BF16),
            pltpu.VMEM((SIDE, BLOCKS, HALF, COLS), BF16),
            pltpu.VMEM((SIDE, BLOCKS, HALF, COLS), BF16),
            pltpu.VMEM((SIDE, 8, 128), F32),
            pltpu.VMEM((SIDE, 8, 128), F32),
            pltpu.VMEM((SIDE, 8, 128), F32),
            pltpu.VMEM((SIDE, 8, 128), F32),
            pltpu.VMEM((BLOCKS, SPAN, 2 * WIDE), F32),
            pltpu.VMEM((BLOCKS, SPAN, WIDE), F32),
            pltpu.VMEM((BLOCKS, NST, WIDE), F32),
            pltpu.VMEM((BLOCKS, NST, WIDE), F32),
            pltpu.VMEM((BLOCKS, NST, WIDE), BF16),
            pltpu.VMEM((BLOCKS, NST, WIDE), BF16),
            pltpu.VMEM((NST, WIDE), F32),
            pltpu.VMEM((NST, WIDE), F32),
            dma((7,)),
            dma((2, 3)),
            dma((2, SIDE)),
            dma((1,)),
            dma((1,)),
            dma((2, 3, BLOCKS)),
            dma((2, SIDE, BLOCKS)),
            dma((2, 3)),
            dma((2, SIDE)),
            dma((2, 3, BLOCKS)),
            dma((2, SIDE, BLOCKS)),
            dma((2, 3)),
            dma((2, SIDE)),
        ],
        compiler_params=pltpu.CompilerParams(
            collective_id=0, has_side_effects=True, vmem_limit_bytes=48 * 1024 * 1024
        ),
        name="encoder",
    )(
        ssm_input, gate_z, proj_forward, proj_backward, step_raw, head_params, skip_gain,
        norm_gain.reshape(1, WIDE), out_weight.reshape(SIDE, SIDE, WIDE, COLS),
    )


def solution(mesh):
    in_specs = (
        P(("batch", "seq"), "chan"),
        P(("batch", "seq"), "chan"),
        P(None, ("batch", "seq"), None),
        P(None, ("batch", "seq"), None),
        P(None, "chan", ("batch", "seq")),
        P(None, None, "chan"),
        P("chan"),
        P("chan"),
        P(None, "chan"),
    )
    out_specs = P(("batch", "seq"), "chan")
    return jax.shard_map(body, mesh=mesh, in_specs=in_specs, out_specs=out_specs, check_vma=False)
```

```python
import jax
import jax.numpy as jnp
from jax import lax
from jax.experimental import pallas as pl
from jax.experimental.pallas import tpu as pltpu
from jax.sharding import PartitionSpec as P

MESH = pl.DeviceIdType.MESH


class Phases:
    def __init__(self):
        self.now = None

    def __call__(self, name):
        if self.now is not None:
            self.now.__exit__(None, None, None)
        self.now = None
        if name is not None:
            self.now = jax.named_scope(name)
            self.now.__enter__()


F32, BF16 = jnp.float32, jnp.bfloat16
SPAN = 256
HALF = 128
BLOCKS = 4
HEADS = 4
WIDE = 256
SIDE = 4
COLS = 128
NST = 128
INNER = 4096
LOG2E = 1.4426950408889634


def iota(shape, dim):
    return lax.broadcasted_iota(jnp.int32, shape, dim)


def dot(a, b):
    return jnp.dot(a, b, preferred_element_type=F32)


def dot_tt(a, b):
    return lax.dot_general(a, b, (((0,), (0,)), ((), ())), preferred_element_type=F32)


def dot_nt(a, b):
    return lax.dot_general(a, b, (((1,), (1,)), ((), ())), preferred_element_type=F32)


def split(v, parts):
    out = []
    for _ in range(parts - 1):
        high = v.astype(BF16).astype(F32)
        out.append(high)
        v = v - high
    out.append(v)
    return out


def tile(i):
    return pl.ds(pl.multiple_of(i * COLS, COLS), COLS)


def kernel(
    x_hbm, z_hbm, pf_hbm, pb_hbm, st_hbm, hp_hbm, skip_hbm, gain_hbm, w_hbm, out_ref,
    hp, skip, gain_ref, xv, zv, pfv, pbv, stv, w1, w2, a1, a2, os1, os2, or1, or2,
    ss1, ss2, so1, so2, yv, sf, sb, ef, eb, payload, carry, ov,
    in_sem, w_send, w_recv, v_send, v_recv, st_send, st_recv,
    a_send, a_recv, r_recv, s_send, s_recv, t_send, t_recv, o_send, o_recv, out_sem,
):
    seq, chan = lax.axis_index("seq"), lax.axis_index("chan")
    my_y, my_x = chan // SIDE, lax.rem(chan, SIDE)
    phase = Phases()

    phase("entry")
    loads = []
    for i, (src, dst) in enumerate(
        (
            (hp_hbm, hp), (st_hbm, stv), (x_hbm, xv), (pf_hbm, pfv), (pb_hbm, pbv),
            (z_hbm, zv), (skip_hbm, skip), (gain_hbm, gain_ref),
            (w_hbm.at[:, my_x], w1.at[:, :, tile(my_x)]), (w_hbm.at[my_y], w2.at[:, :, tile(my_y)]),
        )
    ):
        copy = pltpu.make_async_copy(src, dst, in_sem.at[i])
        copy.start()
        loads.append(copy)

    ys = [lax.rem(my_y + k, SIDE) for k in range(1, SIDE)]
    xs = [lax.rem(my_x + k, SIDE) for k in range(1, SIDE)]
    to_y = [{"chan": v * SIDE + my_x} for v in ys]
    to_x = [{"chan": my_y * SIDE + v} for v in xs]
    other = {"seq": 1 - seq}
    barrier = pltpu.get_barrier_semaphore()
    for dev in to_y + to_x + [other]:
        pl.semaphore_signal(barrier, inc=1, device_id=dev, device_id_type=MESH)
    pl.semaphore_wait(barrier, 7)

    def remote(src, dst, send, recv, dev):
        return pltpu.make_async_remote_copy(
            src_ref=src, dst_ref=dst, send_sem=send, recv_sem=recv,
            device_id=dev, device_id_type=MESH,
        )

    def start(*args):
        remote(*args).start()

    def arrived(ref, send, recv, dev):
        remote(ref, ref, send, recv, dev).wait_recv()

    plans = (
        (a1, w1, os1, or1, ss1, so1, my_y, ys, to_y, my_x, xs, to_x),
        (a2, w2, os2, or2, ss2, so2, my_x, xs, to_x, my_y, ys, to_y),
    )

    half = pl.ds(2 * seq, 2)
    for k in range(3):
        start(w_hbm.at[half, xs[k]], w1.at[half, :, tile(my_x)], w_send.at[0], w_recv.at[0], to_x[k])
        start(w_hbm.at[ys[k], half], w2.at[half, :, tile(my_y)], w_send.at[1], w_recv.at[1], to_y[k])

    def three(w):
        return w.at[pl.ds(0, 2), :, pl.ds(0, 3 * COLS)]

    def pass_weights_on():
        phase("weights1")
        for p, plan in enumerate(plans):
            w, peers, dev = plan[1], plan[10], plan[11]
            arrived(three(w), w_send.at[p], w_recv.at[p], dev[0])
            for k in range(3):
                piece = w.at[half, :, tile(peers[k])]
                start(piece, piece, v_send.at[p], v_recv.at[p], other)

    def all_weights():
        phase("weights2")
        loads[8].wait()
        loads[9].wait()
        for p, plan in enumerate(plans):
            arrived(three(plan[1]), v_send.at[p], v_recv.at[p], other)

    phase("steps")
    loads[0].wait()
    loads[1].wait()
    row8 = iota((8, BLOCKS * SPAN), 0)
    bias = jnp.zeros((8, BLOCKS * SPAN), F32)
    rate = jnp.zeros((8, BLOCKS * SPAN), F32)
    for j in range(8):
        bias = jnp.where(row8 == j, hp[j // 4, 1, j % 4], bias)
        rate = jnp.where(row8 == j, hp[j // 4, 0, j % 4], rate)
    raw = jnp.concatenate([stv[0], stv[1]], axis=0) + bias
    dt_all = jnp.maximum(raw, 0.0) + jnp.log1p(jnp.exp(-jnp.abs(raw)))
    logs = split(-rate * dt_all, 3)
    stacked = jnp.concatenate(
        [part[:, b * SPAN : (b + 1) * SPAN] for b in range(BLOCKS) for part in logs], axis=0
    ).astype(BF16)
    t_of, s_of = iota((SPAN, SPAN), 0), iota((SPAN, SPAN), 1)
    after = t_of >= s_of
    up_to = dot(stacked, jnp.where(t_of <= s_of, 1.0, 0.0).astype(BF16))
    down_to = dot(stacked, jnp.where(after, 1.0, 0.0).astype(BF16))
    is_fwd = iota((8, SPAN), 0) < HEADS
    spread_row, spread_col = iota((16, 2 * WIDE), 0), iota((16, 2 * WIDE), 1)
    spread = jnp.where((spread_row & 7) == (spread_col >> 6), 1.0, 0.0).astype(BF16)
    pick_row, pick_col = iota((32, 128), 0), iota((32, 128), 1)

    def pick(which):
        return jnp.where(((pick_row & 7) == which) & (pick_row < 24), 1.0, 0.0).astype(BF16)

    pick_own = pick(pick_col)
    zero8 = jnp.zeros((8, SPAN), F32)
    chan_row = iota((1, WIDE), 1) >> 6

    def by_head(values):
        row = jnp.zeros((1, WIDE), F32)
        for h in range(HEADS):
            row = jnp.where(chan_row == h, values[h], row)
        return row

    phase("block_states")
    cum2, cprime, dts, decays, grows = [], [], [], [], []
    for copy in loads[2:5]:
        copy.wait()
    for b in range(BLOCKS):
        at, rows = b * 24, slice(b * SPAN, (b + 1) * SPAN)
        c_f = up_to[at : at + 8] + up_to[at + 8 : at + 16] + up_to[at + 16 : at + 24]
        c_b = down_to[at : at + 8] + down_to[at + 8 : at + 16] + down_to[at + 16 : at + 24]
        cum = jnp.where(is_fwd, c_f, c_b)
        end = jnp.where(is_fwd, cum[:, SPAN - 1 : SPAN], cum[:, 0:1])
        dt = dt_all[:, rows]
        e = jnp.exp(cum)
        w = jnp.exp(end - cum) * dt
        c2 = cum * LOG2E
        cum2.append(c2)
        cprime.append(c2 - jnp.log2(dt))
        dts.append(dt)
        grows.append(e)
        decays.append(
            (
                by_head([e[h : h + 1, SPAN - 1 : SPAN] for h in range(HEADS)]),
                by_head([e[HEADS + h : HEADS + h + 1, 0:1] for h in range(HEADS)]),
            )
        )
        w_cols = dot_tt(jnp.concatenate(split(w, 2), axis=0).astype(BF16), spread)
        xb = xv[rows, :].astype(F32)
        sf[b] = dot_tt(pfv[0, rows, :], (xb * w_cols[:, :WIDE]).astype(BF16))
        sb[b] = dot_tt(pbv[0, rows, :], (xb * w_cols[:, WIDE:]).astype(BF16))

    end_f = sf[0]
    for b in range(1, BLOCKS):
        end_f = decays[b][0] * end_f + sf[b]
    end_b = sb[BLOCKS - 1]
    for b in reversed(range(BLOCKS - 1)):
        end_b = decays[b][1] * end_b + sb[b]
    payload[...] = jnp.where(seq == 0, end_f, end_b)
    start(payload, carry, st_send.at[0], st_recv.at[0], other)

    loads[6].wait()
    skip_row = by_head([skip[h] for h in range(HEADS)])
    lane = iota((SPAN, 128), 1)

    def intra(b):
        phase(f"intra{b}")
        rows = slice(b * SPAN, (b + 1) * SPAN)
        b_f, c_f = pfv[0, rows, :], pfv[1, rows, :]
        b_b, c_b = pbv[0, rows, :], pbv[1, rows, :]
        scores = jnp.where(after, dot_nt(c_f, b_f), dot_nt(c_b, b_b))
        cols = dot_tt(jnp.concatenate(split(cum2[b], 3) + [zero8], axis=0).astype(BF16), pick_own)
        dt_cols = dot_tt(jnp.concatenate(split(dts[b], 2), axis=0).astype(BF16), spread[:, WIDE:])
        xb = xv[rows, :]
        same = jnp.sum(c_b.astype(F32) * b_b.astype(F32), axis=1, keepdims=True)
        rest = xb.astype(F32) * (same * dt_cols + skip_row)
        for pair in range(2):
            halves = []
            for h in (2 * pair, 2 * pair + 1):
                gaps = jnp.where(
                    after,
                    cols[:, h : h + 1] - cprime[b][h : h + 1, :],
                    cols[:, 4 + h : 5 + h] - cprime[b][4 + h : 5 + h, :],
                )
                weights = (scores * jnp.exp2(gaps)).astype(BF16)
                halves.append(dot(weights, xb[:, pair * 128 : (pair + 1) * 128]))
            lanes = slice(pair * 128, (pair + 1) * 128)
            yv[b, :, lanes] = jnp.where(lane < 64, halves[0], halves[1]) + rest[:, lanes]

    def enter():
        phase("carry")
        arrived(carry, st_send.at[0], st_recv.at[0], other)
        came = carry[...]
        nothing = jnp.zeros_like(came)
        state = jnp.where(seq == 1, came, nothing)
        for b in range(BLOCKS):
            ef[b] = state.astype(BF16)
            state = decays[b][0] * state + sf[b]
        state = jnp.where(seq == 0, came, nothing)
        for b in reversed(range(BLOCKS)):
            eb[b] = state.astype(BF16)
            state = decays[b][1] * state + sb[b]
        loads[5].wait()
        loads[7].wait()
        ss1[my_y] = jnp.zeros((8, 128), F32)
        ss2[my_x] = jnp.zeros((8, 128), F32)

    ones8 = jnp.ones((8, WIDE), BF16)

    def gate(b):
        phase(f"gate{b}")
        rows = slice(b * SPAN, (b + 1) * SPAN)
        e_cols = dot_tt(jnp.concatenate(split(grows[b], 2), axis=0).astype(BF16), spread)
        inter_f = dot(pfv[1, rows, :], ef[b]) * e_cols[:, :WIDE]
        inter_b = dot(pbv[1, rows, :], eb[b]) * e_cols[:, WIDE:]
        zb = zv[rows, :].astype(F32)
        gated = (yv[b] + inter_f + inter_b) * (zb / (1.0 + jnp.exp(-zb)))
        g = (gated * gain_ref[...]).astype(BF16)
        a1[my_y, b] = g[:HALF]
        a2[my_x, b] = g[HALF:]
        square = split(gated * gated, 2)
        sums = dot_nt(ones8, square[0].astype(BF16)) + dot_nt(ones8, square[1].astype(BF16))
        ss1[my_y, b : b + 1, :] = sums[0:1, :HALF]
        ss2[my_x, b : b + 1, :] = sums[0:1, HALF:]
        for k in (0, 2, 1):
            for p, plan in enumerate(plans):
                a, ss, mine, dev = plan[0], plan[4], plan[6], plan[8]
                if b == BLOCKS - 1:
                    start(ss.at[mine], ss.at[mine], s_send.at[p], s_recv.at[p], dev[k])
                if b == BLOCKS - 1 or k != 1:
                    start(a.at[mine, b], a.at[mine, b], a_send.at[p], a_recv.at[p, b], dev[k])

    def relay(b):
        phase(f"relay{b}")
        for p, plan in enumerate(plans):
            a, src, dev = plan[0], plan[7], plan[8]
            arrived(a.at[pl.ds(0, 2), b], a_send.at[p], a_recv.at[p, b], dev[0])
            for i, k in enumerate((2, 0)):
                half = a.at[src[k], b, pl.ds(i * 64, 64)]
                start(half, half, a_send.at[p], r_recv.at[p, b], dev[2 - k])

    def product(b):
        for p, (a, w, o, dest, ss, so, _, _, dev, mine, peers, back) in enumerate(plans):
            phase(f"wait{b}{p}")
            if b < BLOCKS - 1:
                arrived(a.at[0, b], a_send.at[p], r_recv.at[p, b], dev[0])
            else:
                arrived(a.at[pl.ds(0, 3), b], a_send.at[p], a_recv.at[p, b], dev[0])
            phase(f"product{b}{p}")
            lhs = jnp.concatenate([a[j, b] for j in range(SIDE)], axis=1)
            values = dot(lhs, w[...].reshape(SIDE * WIDE, SIDE * COLS)).astype(BF16)
            for j in range(SIDE):
                o[b, j] = values[:, j * COLS : (j + 1) * COLS]
            for k in range(3):
                start(o.at[b, peers[k]], dest.at[mine, b], o_send.at[p], o_recv.at[p, b], back[k])

    def squares():
        phase("squares")
        for p, (_, _, _, _, ss, so, _, _, dev, mine, _, back) in enumerate(plans):
            arrived(ss.at[pl.ds(0, 3)], s_send.at[p], s_recv.at[p], dev[0])
            so[mine] = ss[0] + ss[1] + ss[2] + ss[3]
            for k in range(3):
                start(so.at[mine], so.at[mine], t_send.at[p], t_recv.at[p], back[k])

    intra(0)
    enter()
    gate(0)
    intra(1)
    gate(1)
    intra(2)
    gate(2)
    pass_weights_on()
    intra(3)
    gate(3)
    relay(0)
    relay(1)
    all_weights()
    relay(2)
    product(0)
    product(1)
    squares()
    product(2)
    product(3)

    phase("scale")
    scales = []
    for p, plan in enumerate(plans):
        so, back = plan[5], plan[11]
        arrived(so.at[pl.ds(0, 3)], t_send.at[p], t_recv.at[p], back[0])
        scale = lax.rsqrt((so[0] + so[1] + so[2] + so[3]) / INNER + 1.0)
        parts = split(scale, 3) + [jnp.zeros((8, 128), F32)]
        scales.append(jnp.concatenate(parts, axis=0).astype(BF16))
    for b in range(BLOCKS):
        phase(f"out{b}")
        pick_b = pick(b)
        for p, (_, _, o, dest, _, _, _, _, _, mine, peers, back) in enumerate(plans):
            scale = dot_tt(scales[p], pick_b)
            arrived(dest.at[pl.ds(0, 3), b], o_send.at[p], o_recv.at[p, b], back[0])
            total = o[b, mine].astype(F32)
            for k in range(3):
                total = total + dest[peers[k], b].astype(F32)
            at = b * SPAN + p * HALF
            ov[at : at + HALF, :] = (total * scale).astype(BF16)
        rows = pl.ds(b * SPAN, SPAN)
        pltpu.make_async_copy(ov.at[rows], out_ref.at[rows], out_sem.at[0]).start()

    phase("drain")
    pltpu.make_async_copy(ov, out_ref, out_sem.at[0]).wait()
    remote(payload, carry, st_send.at[0], st_recv.at[0], other).wait_send()
    for p, (a, w, o, dest, ss, so, _, _, dev, _, _, back) in enumerate(plans):
        for ref, send, recv in (
            (three(w), w_send.at[p], w_recv.at[p]),
            (three(w), v_send.at[p], v_recv.at[p]),
            (a.at[pl.ds(0, 3)], a_send.at[p], a_recv.at[p, 0]),
            (ss.at[pl.ds(0, 3)], s_send.at[p], s_recv.at[p]),
            (so.at[pl.ds(0, 3)], t_send.at[p], t_recv.at[p]),
            (o.at[:, pl.ds(0, 3)], o_send.at[p], o_recv.at[p, 0]),
        ):
            remote(ref, ref, send, recv, dev[0]).wait_send()
    phase(None)


def body(ssm_input, gate_z, proj_forward, proj_backward, step_raw, head_params, skip_gain, norm_gain, out_weight):
    hbm = pl.BlockSpec(memory_space=pltpu.HBM)
    dma = pltpu.SemaphoreType.DMA
    rows = BLOCKS * SPAN
    return pl.pallas_call(
        kernel,
        out_shape=jax.ShapeDtypeStruct((rows, COLS), BF16),
        in_specs=[hbm] * 9,
        out_specs=pl.BlockSpec(memory_space=pl.ANY),
        scratch_shapes=[
            pltpu.SMEM((2, 2, HEADS), F32),
            pltpu.SMEM((HEADS,), F32),
            pltpu.VMEM((1, WIDE), F32),
            pltpu.VMEM((rows, WIDE), BF16),
            pltpu.VMEM((rows, WIDE), BF16),
            pltpu.VMEM((2, rows, NST), BF16),
            pltpu.VMEM((2, rows, NST), BF16),
            pltpu.VMEM((2, HEADS, rows), F32),
            *[pltpu.VMEM((SIDE, WIDE, SIDE * COLS), BF16)] * 2,
            *[pltpu.VMEM((SIDE, BLOCKS, HALF, WIDE), BF16)] * 2,
            *[pltpu.VMEM((BLOCKS, SIDE, HALF, COLS), BF16)] * 2,
            *[pltpu.VMEM((SIDE, BLOCKS, HALF, COLS), BF16)] * 2,
            *[pltpu.VMEM((SIDE, 8, 128), F32)] * 4,
            pltpu.VMEM((BLOCKS, SPAN, WIDE), F32),
            *[pltpu.VMEM((BLOCKS, NST, WIDE), F32)] * 2,
            *[pltpu.VMEM((BLOCKS, NST, WIDE), BF16)] * 2,
            *[pltpu.VMEM((NST, WIDE), F32)] * 2,
            pltpu.VMEM((rows, COLS), BF16),
            dma((10,)),
            *[dma((2,))] * 4,
            *[dma((1,))] * 2,
            dma((2,)),
            dma((2, BLOCKS)),
            dma((2, BLOCKS - 1)),
            *[dma((2,))] * 5,
            dma((2, BLOCKS)),
            dma((1,)),
        ],
        compiler_params=pltpu.CompilerParams(
            collective_id=0, has_side_effects=True, vmem_limit_bytes=48 * 1024 * 1024
        ),
        name="encoder",
    )(*[
        pltpu.with_memory_space_constraint(v, pltpu.HBM)
        for v in (
            ssm_input, gate_z, proj_forward, proj_backward, step_raw, head_params, skip_gain,
            norm_gain.reshape(1, WIDE), out_weight.reshape(SIDE, SIDE, WIDE, COLS),
        )
    ])


def solution(mesh):
    in_specs = (
        P(("batch", "seq"), "chan"),
        P(("batch", "seq"), "chan"),
        P(None, ("batch", "seq"), None),
        P(None, ("batch", "seq"), None),
        P(None, "chan", ("batch", "seq")),
        P(None, None, "chan"),
        P("chan"),
        P("chan"),
        P(None, "chan"),
    )
    out_specs = P(("batch", "seq"), "chan")
    return jax.shard_map(body, mesh=mesh, in_specs=in_specs, out_specs=out_specs, check_vma=False)
```

```python
import jax
import jax.numpy as jnp
from jax import lax
from jax.experimental import pallas as pl
from jax.experimental.pallas import tpu as pltpu
from jax.sharding import PartitionSpec as P

MESH = pl.DeviceIdType.MESH


class Phases:
    def __init__(self):
        self.now = None

    def __call__(self, name):
        if self.now is not None:
            self.now.__exit__(None, None, None)
        self.now = None
        if name is not None:
            self.now = jax.named_scope(name)
            self.now.__enter__()


F32, BF16 = jnp.float32, jnp.bfloat16
SPAN = 256
HALF = 128
BLOCKS = 4
HEADS = 4
WIDE = 256
SIDE = 4
COLS = 128
RELAYED = (0, 1, 2)
NST = 128
INNER = 4096
LOG2E = 1.4426950408889634


def iota(shape, dim):
    return lax.broadcasted_iota(jnp.int32, shape, dim)


def dot(a, b):
    return jnp.dot(a, b, preferred_element_type=F32)


def dot_tt(a, b):
    return lax.dot_general(a, b, (((0,), (0,)), ((), ())), preferred_element_type=F32)


def dot_nt(a, b):
    return lax.dot_general(a, b, (((1,), (1,)), ((), ())), preferred_element_type=F32)


def split(v, parts):
    out = []
    for _ in range(parts - 1):
        high = v.astype(BF16).astype(F32)
        out.append(high)
        v = v - high
    out.append(v)
    return out


def tile(i):
    return pl.ds(pl.multiple_of(i * COLS, COLS), COLS)


def kernel(
    x_hbm, z_hbm, pf_hbm, pb_hbm, st_hbm, hp_hbm, skip_hbm, gain_hbm, w_hbm, out_ref,
    wv, hp, skip, gain_ref, xv, zv, pfv, pbv, stv, w1, w2, a1, a2, os1, os2, or1, or2,
    ss1, ss2, so1, so2, yv, sf, sb, ef, eb, payload, carry,
    in_sem, w_send, w_recv, v_send, v_recv, st_send, st_recv,
    a_send, a_recv, r_recv, s_send, s_recv, t_send, t_recv, o_send, o_recv,
):
    seq, chan = lax.axis_index("seq"), lax.axis_index("chan")
    my_y, my_x = chan // SIDE, lax.rem(chan, SIDE)
    phase = Phases()

    phase("entry")
    ys = [lax.rem(my_y + k, SIDE) for k in range(1, SIDE)]
    xs = [lax.rem(my_x + k, SIDE) for k in range(1, SIDE)]
    to_y = [{"chan": v * SIDE + my_x} for v in ys]
    to_x = [{"chan": my_y * SIDE + v} for v in xs]
    other = {"seq": 1 - seq}
    barrier = pltpu.get_barrier_semaphore()
    for dev in to_y + to_x + [other]:
        pl.semaphore_signal(barrier, inc=1, device_id=dev, device_id_type=MESH)
    loads = []
    for i, (src, dst) in enumerate(
        (
            (w_hbm, wv), (hp_hbm, hp), (st_hbm, stv), (x_hbm, xv), (pf_hbm, pfv), (pb_hbm, pbv),
            (z_hbm, zv), (skip_hbm, skip), (gain_hbm, gain_ref),
            (w_hbm.at[:, my_x], w1.at[:, :, tile(my_x)]), (w_hbm.at[my_y], w2.at[:, :, tile(my_y)]),
        )
    ):
        copy = pltpu.make_async_copy(src, dst, in_sem.at[i])
        copy.start()
        loads.append(copy)
    pl.semaphore_wait(barrier, 7)
    loads[0].wait()

    def remote(src, dst, send, recv, dev):
        return pltpu.make_async_remote_copy(
            src_ref=src, dst_ref=dst, send_sem=send, recv_sem=recv,
            device_id=dev, device_id_type=MESH,
        )

    def start(*args):
        remote(*args).start()

    def arrived(ref, send, recv, dev):
        remote(ref, ref, send, recv, dev).wait_recv()

    plans = (
        (a1, w1, os1, or1, ss1, so1, my_y, ys, to_y, my_x, xs, to_x),
        (a2, w2, os2, or2, ss2, so2, my_x, xs, to_x, my_y, ys, to_y),
    )

    half = pl.ds(2 * seq, 2)
    for k in range(3):
        start(wv.at[half, xs[k]], w1.at[half, :, tile(my_x)], w_send.at[0], w_recv.at[0], to_x[k])
        start(wv.at[ys[k], half], w2.at[half, :, tile(my_y)], w_send.at[1], w_recv.at[1], to_y[k])

    def three(w):
        return w.at[pl.ds(0, 2), :, pl.ds(0, 3 * COLS)]

    def pass_weights_on():
        phase("weights1")
        for p, plan in enumerate(plans):
            w, peers, dev = plan[1], plan[10], plan[11]
            arrived(three(w), w_send.at[p], w_recv.at[p], dev[0])
            for k in range(3):
                piece = w.at[half, :, tile(peers[k])]
                start(piece, piece, v_send.at[p], v_recv.at[p], other)

    def all_weights():
        phase("weights2")
        loads[9].wait()
        loads[10].wait()
        for p, plan in enumerate(plans):
            arrived(three(plan[1]), v_send.at[p], v_recv.at[p], other)

    phase("steps")
    loads[1].wait()
    loads[2].wait()
    row8 = iota((8, BLOCKS * SPAN), 0)
    bias = jnp.zeros((8, BLOCKS * SPAN), F32)
    rate = jnp.zeros((8, BLOCKS * SPAN), F32)
    for j in range(8):
        bias = jnp.where(row8 == j, hp[j // 4, 1, j % 4], bias)
        rate = jnp.where(row8 == j, hp[j // 4, 0, j % 4], rate)
    raw = jnp.concatenate([stv[0], stv[1]], axis=0) + bias
    dt_all = jnp.maximum(raw, 0.0) + jnp.log1p(jnp.exp(-jnp.abs(raw)))
    logs = split(-rate * dt_all, 3)
    stacked = jnp.concatenate(
        [part[:, b * SPAN : (b + 1) * SPAN] for b in range(BLOCKS) for part in logs], axis=0
    ).astype(BF16)
    t_of, s_of = iota((SPAN, SPAN), 0), iota((SPAN, SPAN), 1)
    after = t_of >= s_of
    up_to = dot(stacked, jnp.where(t_of <= s_of, 1.0, 0.0).astype(BF16))
    down_to = dot(stacked, jnp.where(after, 1.0, 0.0).astype(BF16))
    is_fwd = iota((8, SPAN), 0) < HEADS
    spread_row, spread_col = iota((16, 2 * WIDE), 0), iota((16, 2 * WIDE), 1)
    spread = jnp.where((spread_row & 7) == (spread_col >> 6), 1.0, 0.0).astype(BF16)
    pick_row, pick_col = iota((32, 128), 0), iota((32, 128), 1)

    def pick(which):
        return jnp.where(((pick_row & 7) == which) & (pick_row < 24), 1.0, 0.0).astype(BF16)

    pick_own = pick(pick_col)
    zero8 = jnp.zeros((8, SPAN), F32)
    chan_row = iota((1, WIDE), 1) >> 6

    def by_head(values):
        row = jnp.zeros((1, WIDE), F32)
        for h in range(HEADS):
            row = jnp.where(chan_row == h, values[h], row)
        return row

    phase("block_states")
    cum2, cprime, dts, decays, grows = [], [], [], [], []
    for copy in loads[3:6]:
        copy.wait()
    for b in range(BLOCKS):
        at, rows = b * 24, slice(b * SPAN, (b + 1) * SPAN)
        c_f = up_to[at : at + 8] + up_to[at + 8 : at + 16] + up_to[at + 16 : at + 24]
        c_b = down_to[at : at + 8] + down_to[at + 8 : at + 16] + down_to[at + 16 : at + 24]
        cum = jnp.where(is_fwd, c_f, c_b)
        end = jnp.where(is_fwd, cum[:, SPAN - 1 : SPAN], cum[:, 0:1])
        dt = dt_all[:, rows]
        e = jnp.exp(cum)
        w = jnp.exp(end - cum) * dt
        c2 = cum * LOG2E
        cum2.append(c2)
        cprime.append(c2 - jnp.log2(dt))
        dts.append(dt)
        grows.append(e)
        decays.append(
            (
                by_head([e[h : h + 1, SPAN - 1 : SPAN] for h in range(HEADS)]),
                by_head([e[HEADS + h : HEADS + h + 1, 0:1] for h in range(HEADS)]),
            )
        )
        w_cols = dot_tt(jnp.concatenate(split(w, 2), axis=0).astype(BF16), spread)
        xb = xv[rows, :].astype(F32)
        sf[b] = dot_tt(pfv[0, rows, :], (xb * w_cols[:, :WIDE]).astype(BF16))
        sb[b] = dot_tt(pbv[0, rows, :], (xb * w_cols[:, WIDE:]).astype(BF16))

    end_f = sf[0]
    for b in range(1, BLOCKS):
        end_f = decays[b][0] * end_f + sf[b]
    end_b = sb[BLOCKS - 1]
    for b in reversed(range(BLOCKS - 1)):
        end_b = decays[b][1] * end_b + sb[b]
    payload[...] = jnp.where(seq == 0, end_f, end_b)
    start(payload, carry, st_send.at[0], st_recv.at[0], other)

    loads[7].wait()
    skip_row = by_head([skip[h] for h in range(HEADS)])
    lane = iota((SPAN, 128), 1)

    def intra(b):
        phase(f"intra{b}")
        rows = slice(b * SPAN, (b + 1) * SPAN)
        b_f, c_f = pfv[0, rows, :], pfv[1, rows, :]
        b_b, c_b = pbv[0, rows, :], pbv[1, rows, :]
        scores = jnp.where(after, dot_nt(c_f, b_f), dot_nt(c_b, b_b))
        cols = dot_tt(jnp.concatenate(split(cum2[b], 3) + [zero8], axis=0).astype(BF16), pick_own)
        dt_cols = dot_tt(jnp.concatenate(split(dts[b], 2), axis=0).astype(BF16), spread[:, WIDE:])
        xb = xv[rows, :]
        same = jnp.sum(c_b.astype(F32) * b_b.astype(F32), axis=1, keepdims=True)
        rest = xb.astype(F32) * (same * dt_cols + skip_row)
        for pair in range(2):
            halves = []
            for h in (2 * pair, 2 * pair + 1):
                gaps = jnp.where(
                    after,
                    cols[:, h : h + 1] - cprime[b][h : h + 1, :],
                    cols[:, 4 + h : 5 + h] - cprime[b][4 + h : 5 + h, :],
                )
                weights = (scores * jnp.exp2(gaps)).astype(BF16)
                halves.append(dot(weights, xb[:, pair * 128 : (pair + 1) * 128]))
            lanes = slice(pair * 128, (pair + 1) * 128)
            yv[b, :, lanes] = jnp.where(lane < 64, halves[0], halves[1]) + rest[:, lanes]

    def enter():
        phase("carry")
        arrived(carry, st_send.at[0], st_recv.at[0], other)
        came = carry[...]
        nothing = jnp.zeros_like(came)
        state = jnp.where(seq == 1, came, nothing)
        for b in range(BLOCKS):
            ef[b] = state.astype(BF16)
            state = decays[b][0] * state + sf[b]
        state = jnp.where(seq == 0, came, nothing)
        for b in reversed(range(BLOCKS)):
            eb[b] = state.astype(BF16)
            state = decays[b][1] * state + sb[b]
        loads[6].wait()
        loads[8].wait()
        ss1[my_y] = jnp.zeros((8, 128), F32)
        ss2[my_x] = jnp.zeros((8, 128), F32)

    ones8 = jnp.ones((8, WIDE), BF16)

    def gate(b):
        phase(f"gate{b}")
        rows = slice(b * SPAN, (b + 1) * SPAN)
        e_cols = dot_tt(jnp.concatenate(split(grows[b], 2), axis=0).astype(BF16), spread)
        inter_f = dot(pfv[1, rows, :], ef[b]) * e_cols[:, :WIDE]
        inter_b = dot(pbv[1, rows, :], eb[b]) * e_cols[:, WIDE:]
        zb = zv[rows, :].astype(F32)
        gated = (yv[b] + inter_f + inter_b) * (zb / (1.0 + jnp.exp(-zb)))
        g = (gated * gain_ref[...]).astype(BF16)
        a1[my_y, b] = g[:HALF]
        a2[my_x, b] = g[HALF:]
        square = split(gated * gated, 2)
        sums = dot_nt(ones8, square[0].astype(BF16)) + dot_nt(ones8, square[1].astype(BF16))
        ss1[my_y, b : b + 1, :] = sums[0:1, :HALF]
        ss2[my_x, b : b + 1, :] = sums[0:1, HALF:]
        if b == BLOCKS - 1:
            for k in range(3):
                for p, plan in enumerate(plans):
                    ss, mine, dev = plan[4], plan[6], plan[8]
                    start(ss.at[mine], ss.at[mine], s_send.at[p], s_recv.at[p], dev[k])
        for k in (0, 2):
            for p, plan in enumerate(plans):
                a, mine, dev = plan[0], plan[6], plan[8]
                start(a.at[mine, b], a.at[mine, b], a_send.at[p], a_recv.at[p, b], dev[k])

    def send_far(b):
        phase(f"far{b}")
        for p, plan in enumerate(plans):
            a, mine, dev = plan[0], plan[6], plan[8]
            start(a.at[mine, b], a.at[mine, b], a_send.at[p], a_recv.at[p, b], dev[1])

    def relay(b):
        phase(f"relay{b}")
        for p, plan in enumerate(plans):
            a, src, dev = plan[0], plan[7], plan[8]
            arrived(a.at[pl.ds(0, 2), b], a_send.at[p], a_recv.at[p, b], dev[0])
            for i, k in enumerate((2, 0)):
                half = a.at[src[k], b, pl.ds(i * 64, 64)]
                start(half, half, a_send.at[p], r_recv.at[p, b], dev[2 - k])

    def product(b):
        for p, (a, w, o, dest, ss, so, _, _, dev, mine, peers, back) in enumerate(plans):
            phase(f"wait{b}{p}")
            if b in RELAYED:
                arrived(a.at[0, b], a_send.at[p], r_recv.at[p, b], dev[0])
            else:
                arrived(a.at[pl.ds(0, 3), b], a_send.at[p], a_recv.at[p, b], dev[0])
            phase(f"product{b}{p}")
            lhs = jnp.concatenate([a[j, b] for j in range(SIDE)], axis=1)
            values = dot(lhs, w[...].reshape(SIDE * WIDE, SIDE * COLS)).astype(BF16)
            for j in range(SIDE):
                o[b, j] = values[:, j * COLS : (j + 1) * COLS]
            for k in range(3):
                start(o.at[b, peers[k]], dest.at[mine, b], o_send.at[p], o_recv.at[p, b], back[k])

    def squares():
        phase("squares")
        for p, (_, _, _, _, ss, so, _, _, dev, mine, _, back) in enumerate(plans):
            arrived(ss.at[pl.ds(0, 3)], s_send.at[p], s_recv.at[p], dev[0])
            so[mine] = ss[0] + ss[1] + ss[2] + ss[3]
            for k in range(3):
                start(so.at[mine], so.at[mine], t_send.at[p], t_recv.at[p], back[k])

    intra(0)
    enter()
    gate(0)
    intra(1)
    gate(1)
    intra(2)
    gate(2)
    pass_weights_on()
    intra(3)
    gate(3)
    relay(0)
    relay(1)
    all_weights()
    relay(2)
    send_far(3)
    product(0)
    squares()
    product(1)
    product(2)
    product(3)

    phase("scale")
    scales = []
    for p, plan in enumerate(plans):
        so, back = plan[5], plan[11]
        arrived(so.at[pl.ds(0, 3)], t_send.at[p], t_recv.at[p], back[0])
        scale = lax.rsqrt((so[0] + so[1] + so[2] + so[3]) / INNER + 1.0)
        parts = split(scale, 3) + [jnp.zeros((8, 128), F32)]
        scales.append(jnp.concatenate(parts, axis=0).astype(BF16))
    for b in range(BLOCKS):
        phase(f"out{b}")
        pick_b = pick(b)
        for p, (_, _, o, dest, _, _, _, _, _, mine, peers, back) in enumerate(plans):
            scale = dot_tt(scales[p], pick_b)
            arrived(dest.at[pl.ds(0, 3), b], o_send.at[p], o_recv.at[p, b], back[0])
            total = o[b, mine].astype(F32)
            for k in range(3):
                total = total + dest[peers[k], b].astype(F32)
            at = b * SPAN + p * HALF
            out_ref[at : at + HALF, :] = (total * scale).astype(BF16)

    phase("drain")
    remote(payload, carry, st_send.at[0], st_recv.at[0], other).wait_send()
    for p, (a, w, o, dest, ss, so, _, _, dev, _, _, back) in enumerate(plans):
        for ref, send, recv in (
            (three(w), w_send.at[p], w_recv.at[p]),
            (three(w), v_send.at[p], v_recv.at[p]),
            (a.at[pl.ds(0, 3)], a_send.at[p], a_recv.at[p, 0]),
            (ss.at[pl.ds(0, 3)], s_send.at[p], s_recv.at[p]),
            (so.at[pl.ds(0, 3)], t_send.at[p], t_recv.at[p]),
            (o.at[:, pl.ds(0, 3)], o_send.at[p], o_recv.at[p, 0]),
        ):
            remote(ref, ref, send, recv, dev[0]).wait_send()
    phase(None)


def body(ssm_input, gate_z, proj_forward, proj_backward, step_raw, head_params, skip_gain, norm_gain, out_weight):
    hbm = pl.BlockSpec(memory_space=pltpu.HBM)
    dma = pltpu.SemaphoreType.DMA
    rows = BLOCKS * SPAN
    return pl.pallas_call(
        kernel,
        out_shape=jax.ShapeDtypeStruct((rows, COLS), BF16),
        in_specs=[hbm] * 9,
        out_specs=pl.BlockSpec(memory_space=pltpu.VMEM),
        scratch_shapes=[
            pltpu.VMEM((SIDE, SIDE, WIDE, COLS), BF16),
            pltpu.SMEM((2, 2, HEADS), F32),
            pltpu.SMEM((HEADS,), F32),
            pltpu.VMEM((1, WIDE), F32),
            pltpu.VMEM((rows, WIDE), BF16),
            pltpu.VMEM((rows, WIDE), BF16),
            pltpu.VMEM((2, rows, NST), BF16),
            pltpu.VMEM((2, rows, NST), BF16),
            pltpu.VMEM((2, HEADS, rows), F32),
            *[pltpu.VMEM((SIDE, WIDE, SIDE * COLS), BF16)] * 2,
            *[pltpu.VMEM((SIDE, BLOCKS, HALF, WIDE), BF16)] * 2,
            *[pltpu.VMEM((BLOCKS, SIDE, HALF, COLS), BF16)] * 2,
            *[pltpu.VMEM((SIDE, BLOCKS, HALF, COLS), BF16)] * 2,
            *[pltpu.VMEM((SIDE, 8, 128), F32)] * 4,
            pltpu.VMEM((BLOCKS, SPAN, WIDE), F32),
            *[pltpu.VMEM((BLOCKS, NST, WIDE), F32)] * 2,
            *[pltpu.VMEM((BLOCKS, NST, WIDE), BF16)] * 2,
            *[pltpu.VMEM((NST, WIDE), F32)] * 2,
            dma((11,)),
            *[dma((2,))] * 4,
            *[dma((1,))] * 2,
            dma((2,)),
            dma((2, BLOCKS)),
            dma((2, BLOCKS)),
            *[dma((2,))] * 5,
            dma((2, BLOCKS)),
        ],
        compiler_params=pltpu.CompilerParams(
            collective_id=0, has_side_effects=True, vmem_limit_bytes=48 * 1024 * 1024
        ),
        name="encoder",
    )(*[
        pltpu.with_memory_space_constraint(v, pltpu.HBM)
        for v in (
            ssm_input, gate_z, proj_forward, proj_backward, step_raw, head_params, skip_gain,
            norm_gain.reshape(1, WIDE), out_weight.reshape(SIDE, SIDE, WIDE, COLS),
        )
    ])


def solution(mesh):
    in_specs = (
        P(("batch", "seq"), "chan"),
        P(("batch", "seq"), "chan"),
        P(None, ("batch", "seq"), None),
        P(None, ("batch", "seq"), None),
        P(None, "chan", ("batch", "seq")),
        P(None, None, "chan"),
        P("chan"),
        P("chan"),
        P(None, "chan"),
    )
    out_specs = P(("batch", "seq"), "chan")
    return jax.shard_map(body, mesh=mesh, in_specs=in_specs, out_specs=out_specs, check_vma=False)
```

```python
import jax
import jax.numpy as jnp
from jax import lax
from jax.experimental import pallas as pl
from jax.experimental.pallas import tpu as pltpu
from jax.sharding import PartitionSpec as P

MESH = pl.DeviceIdType.MESH


class Phases:
    def __init__(self):
        self.now = None

    def __call__(self, name):
        if self.now is not None:
            self.now.__exit__(None, None, None)
        self.now = None
        if name is not None:
            self.now = jax.named_scope(name)
            self.now.__enter__()


F32, BF16 = jnp.float32, jnp.bfloat16
SPAN = 256
HALF = 128
BLOCKS = 4
HEADS = 4
WIDE = 256
SIDE = 4
COLS = 128
RELAYED = (0, 1, 2)
NST = 128
INNER = 4096
LOG2E = 1.4426950408889634


def iota(shape, dim):
    return lax.broadcasted_iota(jnp.int32, shape, dim)


def dot(a, b):
    return jnp.dot(a, b, preferred_element_type=F32)


def dot_tt(a, b):
    return lax.dot_general(a, b, (((0,), (0,)), ((), ())), preferred_element_type=F32)


def dot_nt(a, b):
    return lax.dot_general(a, b, (((1,), (1,)), ((), ())), preferred_element_type=F32)


def split(v, parts):
    out = []
    for _ in range(parts - 1):
        high = v.astype(BF16).astype(F32)
        out.append(high)
        v = v - high
    out.append(v)
    return out


def tile(i):
    return pl.ds(pl.multiple_of(i * COLS, COLS), COLS)


def kernel(
    x_hbm, z_hbm, pf_hbm, pb_hbm, st_hbm, hp_hbm, skip_hbm, gain_hbm, w_hbm, out_ref,
    wv, hp, skip, gain_ref, xv, zv, pfv, pbv, stv, w1, w2, a1, a2, os1, os2, or1, or2,
    ss1, ss2, so1, so2, yv, sf, sb, ef, eb, payload, carry,
    in_sem, w_send, w_recv, v_send, v_recv, st_send, st_recv,
    a_send, a_recv, r_recv, s_send, s_recv, t_send, t_recv, o_send, o_recv,
):
    seq, chan = lax.axis_index("seq"), lax.axis_index("chan")
    my_y, my_x = chan // SIDE, lax.rem(chan, SIDE)
    phase = Phases()

    phase("entry")
    ys = [lax.rem(my_y + k, SIDE) for k in range(1, SIDE)]
    xs = [lax.rem(my_x + k, SIDE) for k in range(1, SIDE)]
    to_y = [{"chan": v * SIDE + my_x} for v in ys]
    to_x = [{"chan": my_y * SIDE + v} for v in xs]
    other = {"seq": 1 - seq}
    barrier = pltpu.get_barrier_semaphore()
    for dev in to_y + to_x + [other]:
        pl.semaphore_signal(barrier, inc=1, device_id=dev, device_id_type=MESH)
    loads = []
    for i, (src, dst) in enumerate(
        (
            (w_hbm, wv), (hp_hbm, hp), (st_hbm, stv), (x_hbm, xv), (pf_hbm, pfv), (pb_hbm, pbv),
            (z_hbm, zv), (skip_hbm, skip), (gain_hbm, gain_ref),
            (w_hbm.at[:, my_x], w1.at[:, :, tile(my_x)]), (w_hbm.at[my_y], w2.at[:, :, tile(my_y)]),
        )
    ):
        copy = pltpu.make_async_copy(src, dst, in_sem.at[i])
        copy.start()
        loads.append(copy)
    pl.semaphore_wait(barrier, 7)
    loads[0].wait()

    def remote(src, dst, send, recv, dev):
        return pltpu.make_async_remote_copy(
            src_ref=src, dst_ref=dst, send_sem=send, recv_sem=recv,
            device_id=dev, device_id_type=MESH,
        )

    def start(*args):
        remote(*args).start()

    def arrived(ref, send, recv, dev):
        remote(ref, ref, send, recv, dev).wait_recv()

    plans = (
        (a1, w1, os1, or1, ss1, so1, my_y, ys, to_y, my_x, xs, to_x),
        (a2, w2, os2, or2, ss2, so2, my_x, xs, to_x, my_y, ys, to_y),
    )

    half = pl.ds(2 * seq, 2)
    for k in (1, 0, 2):
        start(wv.at[half, xs[k]], w1.at[half, :, tile(my_x)], w_send.at[0], w_recv.at[0], to_x[k])
        start(wv.at[ys[k], half], w2.at[half, :, tile(my_y)], w_send.at[1], w_recv.at[1], to_y[k])

    def three(w):
        return w.at[pl.ds(0, 2), :, pl.ds(0, 3 * COLS)]

    def pass_weights_on():
        phase("weights1")
        for p, plan in enumerate(plans):
            w, peers, dev = plan[1], plan[10], plan[11]
            arrived(three(w), w_send.at[p], w_recv.at[p], dev[0])
            for k in range(3):
                piece = w.at[half, :, tile(peers[k])]
                start(piece, piece, v_send.at[p], v_recv.at[p], other)

    def all_weights():
        phase("weights2")
        loads[9].wait()
        loads[10].wait()
        for p, plan in enumerate(plans):
            arrived(three(plan[1]), v_send.at[p], v_recv.at[p], other)

    phase("steps")
    loads[1].wait()
    loads[2].wait()
    row8 = iota((8, BLOCKS * SPAN), 0)
    bias = jnp.zeros((8, BLOCKS * SPAN), F32)
    rate = jnp.zeros((8, BLOCKS * SPAN), F32)
    for j in range(8):
        bias = jnp.where(row8 == j, hp[j // 4, 1, j % 4], bias)
        rate = jnp.where(row8 == j, hp[j // 4, 0, j % 4], rate)
    raw = jnp.concatenate([stv[0], stv[1]], axis=0) + bias
    dt_all = jnp.maximum(raw, 0.0) + jnp.log1p(jnp.exp(-jnp.abs(raw)))
    logs = split(-rate * dt_all, 3)
    stacked = jnp.concatenate(
        [part[:, b * SPAN : (b + 1) * SPAN] for b in range(BLOCKS) for part in logs], axis=0
    ).astype(BF16)
    t_of, s_of = iota((SPAN, SPAN), 0), iota((SPAN, SPAN), 1)
    after = t_of >= s_of
    up_to = dot(stacked, jnp.where(t_of <= s_of, 1.0, 0.0).astype(BF16))
    down_to = dot(stacked, jnp.where(after, 1.0, 0.0).astype(BF16))
    is_fwd = iota((8, SPAN), 0) < HEADS
    spread_row, spread_col = iota((16, 2 * WIDE), 0), iota((16, 2 * WIDE), 1)
    spread = jnp.where((spread_row & 7) == (spread_col >> 6), 1.0, 0.0).astype(BF16)
    pick_row, pick_col = iota((32, 128), 0), iota((32, 128), 1)

    def pick(which):
        return jnp.where(((pick_row & 7) == which) & (pick_row < 24), 1.0, 0.0).astype(BF16)

    pick_own = pick(pick_col)
    zero8 = jnp.zeros((8, SPAN), F32)
    chan_row = iota((1, WIDE), 1) >> 6

    def by_head(values):
        row = jnp.zeros((1, WIDE), F32)
        for h in range(HEADS):
            row = jnp.where(chan_row == h, values[h], row)
        return row

    phase("block_states")
    cum2, cprime, dts, decays, grows = [], [], [], [], []
    for copy in loads[3:6]:
        copy.wait()
    for b in range(BLOCKS):
        at, rows = b * 24, slice(b * SPAN, (b + 1) * SPAN)
        c_f = up_to[at : at + 8] + up_to[at + 8 : at + 16] + up_to[at + 16 : at + 24]
        c_b = down_to[at : at + 8] + down_to[at + 8 : at + 16] + down_to[at + 16 : at + 24]
        cum = jnp.where(is_fwd, c_f, c_b)
        end = jnp.where(is_fwd, cum[:, SPAN - 1 : SPAN], cum[:, 0:1])
        dt = dt_all[:, rows]
        e = jnp.exp(cum)
        w = jnp.exp(end - cum) * dt
        c2 = cum * LOG2E
        cum2.append(c2)
        cprime.append(c2 - jnp.log2(dt))
        dts.append(dt)
        grows.append(e)
        decays.append(
            (
                by_head([e[h : h + 1, SPAN - 1 : SPAN] for h in range(HEADS)]),
                by_head([e[HEADS + h : HEADS + h + 1, 0:1] for h in range(HEADS)]),
            )
        )
        w_cols = dot_tt(jnp.concatenate(split(w, 2), axis=0).astype(BF16), spread)
        xb = xv[rows, :].astype(F32)
        sf[b] = dot_tt(pfv[0, rows, :], (xb * w_cols[:, :WIDE]).astype(BF16))
        sb[b] = dot_tt(pbv[0, rows, :], (xb * w_cols[:, WIDE:]).astype(BF16))

    end_f = sf[0]
    for b in range(1, BLOCKS):
        end_f = decays[b][0] * end_f + sf[b]
    end_b = sb[BLOCKS - 1]
    for b in reversed(range(BLOCKS - 1)):
        end_b = decays[b][1] * end_b + sb[b]
    payload[...] = jnp.where(seq == 0, end_f, end_b)
    start(payload, carry, st_send.at[0], st_recv.at[0], other)

    loads[7].wait()
    skip_row = by_head([skip[h] for h in range(HEADS)])
    lane = iota((SPAN, 128), 1)

    def intra(b):
        phase(f"intra{b}")
        rows = slice(b * SPAN, (b + 1) * SPAN)
        b_f, c_f = pfv[0, rows, :], pfv[1, rows, :]
        b_b, c_b = pbv[0, rows, :], pbv[1, rows, :]
        scores = jnp.where(after, dot_nt(c_f, b_f), dot_nt(c_b, b_b))
        cols = dot_tt(jnp.concatenate(split(cum2[b], 3) + [zero8], axis=0).astype(BF16), pick_own)
        dt_cols = dot_tt(jnp.concatenate(split(dts[b], 2), axis=0).astype(BF16), spread[:, WIDE:])
        xb = xv[rows, :]
        same = jnp.sum(c_b.astype(F32) * b_b.astype(F32), axis=1, keepdims=True)
        rest = xb.astype(F32) * (same * dt_cols + skip_row)
        for pair in range(2):
            halves = []
            for h in (2 * pair, 2 * pair + 1):
                gaps = jnp.where(
                    after,
                    cols[:, h : h + 1] - cprime[b][h : h + 1, :],
                    cols[:, 4 + h : 5 + h] - cprime[b][4 + h : 5 + h, :],
                )
                weights = (scores * jnp.exp2(gaps)).astype(BF16)
                halves.append(dot(weights, xb[:, pair * 128 : (pair + 1) * 128]))
            lanes = slice(pair * 128, (pair + 1) * 128)
            yv[b, :, lanes] = jnp.where(lane < 64, halves[0], halves[1]) + rest[:, lanes]

    def enter():
        phase("carry")
        arrived(carry, st_send.at[0], st_recv.at[0], other)
        came = carry[...]
        nothing = jnp.zeros_like(came)
        state = jnp.where(seq == 1, came, nothing)
        for b in range(BLOCKS):
            ef[b] = state.astype(BF16)
            state = decays[b][0] * state + sf[b]
        state = jnp.where(seq == 0, came, nothing)
        for b in reversed(range(BLOCKS)):
            eb[b] = state.astype(BF16)
            state = decays[b][1] * state + sb[b]
        loads[6].wait()
        loads[8].wait()
        ss1[my_y] = jnp.zeros((8, 128), F32)
        ss2[my_x] = jnp.zeros((8, 128), F32)

    ones8 = jnp.ones((8, WIDE), BF16)

    def gate(b):
        phase(f"gate{b}")
        rows = slice(b * SPAN, (b + 1) * SPAN)
        e_cols = dot_tt(jnp.concatenate(split(grows[b], 2), axis=0).astype(BF16), spread)
        inter_f = dot(pfv[1, rows, :], ef[b]) * e_cols[:, :WIDE]
        inter_b = dot(pbv[1, rows, :], eb[b]) * e_cols[:, WIDE:]
        zb = zv[rows, :].astype(F32)
        gated = (yv[b] + inter_f + inter_b) * (zb / (1.0 + jnp.exp(-zb)))
        g = (gated * gain_ref[...]).astype(BF16)
        a1[my_y, b] = g[:HALF]
        a2[my_x, b] = g[HALF:]
        square = split(gated * gated, 2)
        sums = dot_nt(ones8, square[0].astype(BF16)) + dot_nt(ones8, square[1].astype(BF16))
        ss1[my_y, b : b + 1, :] = sums[0:1, :HALF]
        ss2[my_x, b : b + 1, :] = sums[0:1, HALF:]
        if b == BLOCKS - 1:
            for k in range(3):
                for p, plan in enumerate(plans):
                    ss, mine, dev = plan[4], plan[6], plan[8]
                    start(ss.at[mine], ss.at[mine], s_send.at[p], s_recv.at[p], dev[k])
        for k in (0, 2):
            for p, plan in enumerate(plans):
                a, mine, dev = plan[0], plan[6], plan[8]
                start(a.at[mine, b], a.at[mine, b], a_send.at[p], a_recv.at[p, b], dev[k])

    def send_far(b):
        phase(f"far{b}")
        for p, plan in enumerate(plans):
            a, mine, dev = plan[0], plan[6], plan[8]
            start(a.at[mine, b], a.at[mine, b], a_send.at[p], a_recv.at[p, b], dev[1])

    def relay(b):
        phase(f"relay{b}")
        for p, plan in enumerate(plans):
            a, src, dev = plan[0], plan[7], plan[8]
            arrived(a.at[pl.ds(0, 2), b], a_send.at[p], a_recv.at[p, b], dev[0])
            for i, k in enumerate((2, 0)):
                half = a.at[src[k], b, pl.ds(i * 64, 64)]
                start(half, half, a_send.at[p], r_recv.at[p, b], dev[2 - k])

    def product(b):
        for p, (a, w, o, dest, ss, so, _, _, dev, mine, peers, back) in enumerate(plans):
            phase(f"wait{b}{p}")
            if b in RELAYED:
                arrived(a.at[0, b], a_send.at[p], r_recv.at[p, b], dev[0])
            else:
                arrived(a.at[pl.ds(0, 3), b], a_send.at[p], a_recv.at[p, b], dev[0])
            phase(f"product{b}{p}")
            lhs = jnp.concatenate([a[j, b] for j in range(SIDE)], axis=1)
            values = dot(lhs, w[...].reshape(SIDE * WIDE, SIDE * COLS)).astype(BF16)
            for j in range(SIDE):
                o[b, j] = values[:, j * COLS : (j + 1) * COLS]
            for k in (1, 0, 2):
                start(o.at[b, peers[k]], dest.at[mine, b], o_send.at[p], o_recv.at[p, b], back[k])

    def squares():
        phase("squares")
        for p, (_, _, _, _, ss, so, _, _, dev, mine, _, back) in enumerate(plans):
            arrived(ss.at[pl.ds(0, 3)], s_send.at[p], s_recv.at[p], dev[0])
            so[mine] = ss[0] + ss[1] + ss[2] + ss[3]
            for k in range(3):
                start(so.at[mine], so.at[mine], t_send.at[p], t_recv.at[p], back[k])

    intra(0)
    enter()
    gate(0)
    intra(1)
    gate(1)
    intra(2)
    gate(2)
    pass_weights_on()
    intra(3)
    gate(3)
    relay(0)
    relay(1)
    all_weights()
    relay(2)
    send_far(3)
    product(0)
    squares()
    product(1)
    product(2)
    product(3)

    phase("scale")
    scales = []
    for p, plan in enumerate(plans):
        so, back = plan[5], plan[11]
        arrived(so.at[pl.ds(0, 3)], t_send.at[p], t_recv.at[p], back[0])
        scale = lax.rsqrt((so[0] + so[1] + so[2] + so[3]) / INNER + 1.0)
        parts = split(scale, 3) + [jnp.zeros((8, 128), F32)]
        scales.append(jnp.concatenate(parts, axis=0).astype(BF16))
    for b in range(BLOCKS):
        phase(f"out{b}")
        pick_b = pick(b)
        for p, (_, _, o, dest, _, _, _, _, _, mine, peers, back) in enumerate(plans):
            scale = dot_tt(scales[p], pick_b)
            arrived(dest.at[pl.ds(0, 3), b], o_send.at[p], o_recv.at[p, b], back[0])
            total = o[b, mine].astype(F32)
            for k in range(3):
                total = total + dest[peers[k], b].astype(F32)
            at = b * SPAN + p * HALF
            out_ref[at : at + HALF, :] = (total * scale).astype(BF16)

    phase("drain")
    remote(payload, carry, st_send.at[0], st_recv.at[0], other).wait_send()
    for p, (a, w, o, dest, ss, so, _, _, dev, _, _, back) in enumerate(plans):
        for ref, send, recv in (
            (three(w), w_send.at[p], w_recv.at[p]),
            (three(w), v_send.at[p], v_recv.at[p]),
            (a.at[pl.ds(0, 3)], a_send.at[p], a_recv.at[p, 0]),
            (ss.at[pl.ds(0, 3)], s_send.at[p], s_recv.at[p]),
            (so.at[pl.ds(0, 3)], t_send.at[p], t_recv.at[p]),
            (o.at[:, pl.ds(0, 3)], o_send.at[p], o_recv.at[p, 0]),
        ):
            remote(ref, ref, send, recv, dev[0]).wait_send()
    phase(None)


def body(ssm_input, gate_z, proj_forward, proj_backward, step_raw, head_params, skip_gain, norm_gain, out_weight):
    hbm = pl.BlockSpec(memory_space=pltpu.HBM)
    dma = pltpu.SemaphoreType.DMA
    rows = BLOCKS * SPAN
    return pl.pallas_call(
        kernel,
        out_shape=jax.ShapeDtypeStruct((rows, COLS), BF16),
        in_specs=[hbm] * 9,
        out_specs=pl.BlockSpec(memory_space=pltpu.VMEM),
        scratch_shapes=[
            pltpu.VMEM((SIDE, SIDE, WIDE, COLS), BF16),
            pltpu.SMEM((2, 2, HEADS), F32),
            pltpu.SMEM((HEADS,), F32),
            pltpu.VMEM((1, WIDE), F32),
            pltpu.VMEM((rows, WIDE), BF16),
            pltpu.VMEM((rows, WIDE), BF16),
            pltpu.VMEM((2, rows, NST), BF16),
            pltpu.VMEM((2, rows, NST), BF16),
            pltpu.VMEM((2, HEADS, rows), F32),
            *[pltpu.VMEM((SIDE, WIDE, SIDE * COLS), BF16)] * 2,
            *[pltpu.VMEM((SIDE, BLOCKS, HALF, WIDE), BF16)] * 2,
            *[pltpu.VMEM((BLOCKS, SIDE, HALF, COLS), BF16)] * 2,
            *[pltpu.VMEM((SIDE, BLOCKS, HALF, COLS), BF16)] * 2,
            *[pltpu.VMEM((SIDE, 8, 128), F32)] * 4,
            pltpu.VMEM((BLOCKS, SPAN, WIDE), F32),
            *[pltpu.VMEM((BLOCKS, NST, WIDE), F32)] * 2,
            *[pltpu.VMEM((BLOCKS, NST, WIDE), BF16)] * 2,
            *[pltpu.VMEM((NST, WIDE), F32)] * 2,
            dma((11,)),
            *[dma((2,))] * 4,
            *[dma((1,))] * 2,
            dma((2,)),
            dma((2, BLOCKS)),
            dma((2, BLOCKS)),
            *[dma((2,))] * 5,
            dma((2, BLOCKS)),
        ],
        compiler_params=pltpu.CompilerParams(
            collective_id=0, has_side_effects=True, vmem_limit_bytes=48 * 1024 * 1024
        ),
        name="encoder",
    )(*[
        pltpu.with_memory_space_constraint(v, pltpu.HBM)
        for v in (
            ssm_input, gate_z, proj_forward, proj_backward, step_raw, head_params, skip_gain,
            norm_gain.reshape(1, WIDE), out_weight.reshape(SIDE, SIDE, WIDE, COLS),
        )
    ])


def solution(mesh):
    in_specs = (
        P(("batch", "seq"), "chan"),
        P(("batch", "seq"), "chan"),
        P(None, ("batch", "seq"), None),
        P(None, ("batch", "seq"), None),
        P(None, "chan", ("batch", "seq")),
        P(None, None, "chan"),
        P("chan"),
        P("chan"),
        P(None, "chan"),
    )
    out_specs = P(("batch", "seq"), "chan")
    return jax.shard_map(body, mesh=mesh, in_specs=in_specs, out_specs=out_specs, check_vma=False)
```

```python
import jax
import jax.numpy as jnp
from jax import lax
from jax.experimental import pallas as pl
from jax.experimental.pallas import tpu as pltpu
from jax.sharding import PartitionSpec as P

MESH = pl.DeviceIdType.MESH


class Phases:
    def __init__(self):
        self.now = None

    def __call__(self, name):
        if self.now is not None:
            self.now.__exit__(None, None, None)
        self.now = None
        if name is not None:
            self.now = jax.named_scope(name)
            self.now.__enter__()


F32, BF16 = jnp.float32, jnp.bfloat16
SPAN = 256
HALF = 128
BLOCKS = 4
HEADS = 4
WIDE = 256
SIDE = 4
COLS = 128
RELAYED = (0, 1, 2)
NST = 128
INNER = 4096
LOG2E = 1.4426950408889634


def iota(shape, dim):
    return lax.broadcasted_iota(jnp.int32, shape, dim)


def dot(a, b):
    return jnp.dot(a, b, preferred_element_type=F32)


def dot_tt(a, b):
    return lax.dot_general(a, b, (((0,), (0,)), ((), ())), preferred_element_type=F32)


def dot_nt(a, b):
    return lax.dot_general(a, b, (((1,), (1,)), ((), ())), preferred_element_type=F32)


def split(v, parts):
    out = []
    for _ in range(parts - 1):
        high = v.astype(BF16).astype(F32)
        out.append(high)
        v = v - high
    out.append(v)
    return out


def tile(i):
    return pl.ds(pl.multiple_of(i * COLS, COLS), COLS)


def kernel(
    x_hbm, z_hbm, pf_hbm, pb_hbm, st_hbm, hp_hbm, skip_hbm, gain_hbm, w_hbm, out_ref,
    wv, hp, skip, gain_ref, xv, zv, pfv, pbv, stv, w1, w2, a1, a2, os1, os2, or1, or2,
    ss1, ss2, so1, so2, yv, sf, sb, ef, eb, payload, carry,
    in_sem, w_send, w_recv, v_send, v_recv, st_send, st_recv,
    a_send, a_recv, r_recv, s_send, s_recv, t_send, t_recv, o_send, o_recv,
):
    seq, chan = lax.axis_index("seq"), lax.axis_index("chan")
    my_y, my_x = chan // SIDE, lax.rem(chan, SIDE)
    phase = Phases()

    phase("entry")
    ys = [lax.rem(my_y + k, SIDE) for k in range(1, SIDE)]
    xs = [lax.rem(my_x + k, SIDE) for k in range(1, SIDE)]
    to_y = [{"chan": v * SIDE + my_x} for v in ys]
    to_x = [{"chan": my_y * SIDE + v} for v in xs]
    other = {"seq": 1 - seq}
    barrier = pltpu.get_barrier_semaphore()
    for dev in to_y + to_x + [other]:
        pl.semaphore_signal(barrier, inc=1, device_id=dev, device_id_type=MESH)
    loads = []
    for i, (src, dst) in enumerate(
        (
            (w_hbm, wv), (hp_hbm, hp), (st_hbm, stv), (x_hbm, xv), (pf_hbm, pfv), (pb_hbm, pbv),
            (z_hbm, zv), (skip_hbm, skip), (gain_hbm, gain_ref),
            (w_hbm.at[:, my_x], w1.at[:, :, tile(my_x)]), (w_hbm.at[my_y], w2.at[:, :, tile(my_y)]),
        )
    ):
        copy = pltpu.make_async_copy(src, dst, in_sem.at[i])
        copy.start()
        loads.append(copy)
    pl.semaphore_wait(barrier, 7)
    loads[0].wait()

    def remote(src, dst, send, recv, dev):
        return pltpu.make_async_remote_copy(
            src_ref=src, dst_ref=dst, send_sem=send, recv_sem=recv,
            device_id=dev, device_id_type=MESH,
        )

    def start(*args):
        remote(*args).start()

    def arrived(ref, send, recv, dev):
        remote(ref, ref, send, recv, dev).wait_recv()

    plans = (
        (a1, w1, os1, or1, ss1, so1, my_y, ys, to_y, my_x, xs, to_x),
        (a2, w2, os2, or2, ss2, so2, my_x, xs, to_x, my_y, ys, to_y),
    )

    half = pl.ds(2 * seq, 2)
    for k in (1, 0, 2):
        start(wv.at[half, xs[k]], w1.at[half, :, tile(my_x)], w_send.at[0], w_recv.at[0], to_x[k])
        start(wv.at[ys[k], half], w2.at[half, :, tile(my_y)], w_send.at[1], w_recv.at[1], to_y[k])

    def three(w):
        return w.at[pl.ds(0, 2), :, pl.ds(0, 3 * COLS)]

    def pass_weights_on():
        phase("weights1")
        for p, plan in enumerate(plans):
            w, peers, dev = plan[1], plan[10], plan[11]
            arrived(three(w), w_send.at[p], w_recv.at[p], dev[0])
            for k in range(3):
                piece = w.at[half, :, tile(peers[k])]
                start(piece, piece, v_send.at[p], v_recv.at[p], other)

    def all_weights():
        phase("weights2")
        loads[9].wait()
        loads[10].wait()
        for p, plan in enumerate(plans):
            arrived(three(plan[1]), v_send.at[p], v_recv.at[p], other)

    phase("steps")
    loads[1].wait()
    loads[2].wait()
    row8 = iota((8, BLOCKS * SPAN), 0)
    bias = jnp.zeros((8, BLOCKS * SPAN), F32)
    rate = jnp.zeros((8, BLOCKS * SPAN), F32)
    for j in range(8):
        bias = jnp.where(row8 == j, hp[j // 4, 1, j % 4], bias)
        rate = jnp.where(row8 == j, hp[j // 4, 0, j % 4], rate)
    raw = jnp.concatenate([stv[0], stv[1]], axis=0) + bias
    dt_all = jnp.maximum(raw, 0.0) + jnp.log1p(jnp.exp(-jnp.abs(raw)))
    logs = split(-rate * dt_all, 3)
    stacked = jnp.concatenate(
        [part[:, b * SPAN : (b + 1) * SPAN] for b in range(BLOCKS) for part in logs], axis=0
    ).astype(BF16)
    t_of, s_of = iota((SPAN, SPAN), 0), iota((SPAN, SPAN), 1)
    after = t_of >= s_of
    up_to = dot(stacked, jnp.where(t_of <= s_of, 1.0, 0.0).astype(BF16))
    down_to = dot(stacked, jnp.where(after, 1.0, 0.0).astype(BF16))
    is_fwd = iota((8, SPAN), 0) < HEADS
    spread_row, spread_col = iota((16, 2 * WIDE), 0), iota((16, 2 * WIDE), 1)
    spread = jnp.where((spread_row & 7) == (spread_col >> 6), 1.0, 0.0).astype(BF16)
    pick_row, pick_col = iota((32, 128), 0), iota((32, 128), 1)

    def pick(which):
        return jnp.where(((pick_row & 7) == which) & (pick_row < 24), 1.0, 0.0).astype(BF16)

    pick_own = pick(pick_col)
    zero8 = jnp.zeros((8, SPAN), F32)
    chan_row = iota((1, WIDE), 1) >> 6

    def by_head(values):
        row = jnp.zeros((1, WIDE), F32)
        for h in range(HEADS):
            row = jnp.where(chan_row == h, values[h], row)
        return row

    phase("block_states")
    cum2, cprime, dts, decays, grows = [], [], [], [], []
    for copy in loads[3:6]:
        copy.wait()
    for b in range(BLOCKS):
        at, rows = b * 24, slice(b * SPAN, (b + 1) * SPAN)
        c_f = up_to[at : at + 8] + up_to[at + 8 : at + 16] + up_to[at + 16 : at + 24]
        c_b = down_to[at : at + 8] + down_to[at + 8 : at + 16] + down_to[at + 16 : at + 24]
        cum = jnp.where(is_fwd, c_f, c_b)
        end = jnp.where(is_fwd, cum[:, SPAN - 1 : SPAN], cum[:, 0:1])
        dt = dt_all[:, rows]
        e = jnp.exp(cum)
        w = jnp.exp(end - cum) * dt
        c2 = cum * LOG2E
        cum2.append(c2)
        cprime.append(c2 - jnp.log2(dt))
        dts.append(dt)
        grows.append(e)
        decays.append(
            (
                by_head([e[h : h + 1, SPAN - 1 : SPAN] for h in range(HEADS)]),
                by_head([e[HEADS + h : HEADS + h + 1, 0:1] for h in range(HEADS)]),
            )
        )
        w_cols = dot_tt(jnp.concatenate(split(w, 2), axis=0).astype(BF16), spread)
        xb = xv[rows, :].astype(F32)
        sf[b] = dot_tt(pfv[0, rows, :], (xb * w_cols[:, :WIDE]).astype(BF16))
        sb[b] = dot_tt(pbv[0, rows, :], (xb * w_cols[:, WIDE:]).astype(BF16))

    end_f = sf[0]
    for b in range(1, BLOCKS):
        end_f = decays[b][0] * end_f + sf[b]
    end_b = sb[BLOCKS - 1]
    for b in reversed(range(BLOCKS - 1)):
        end_b = decays[b][1] * end_b + sb[b]
    payload[...] = jnp.where(seq == 0, end_f, end_b)
    start(payload, carry, st_send.at[0], st_recv.at[0], other)

    loads[7].wait()
    skip_row = by_head([skip[h] for h in range(HEADS)])
    lane = iota((SPAN, 128), 1)

    def intra(b):
        phase(f"intra{b}")
        rows = slice(b * SPAN, (b + 1) * SPAN)
        b_f, c_f = pfv[0, rows, :], pfv[1, rows, :]
        b_b, c_b = pbv[0, rows, :], pbv[1, rows, :]
        scores = jnp.where(after, dot_nt(c_f, b_f), dot_nt(c_b, b_b))
        cols = dot_tt(jnp.concatenate(split(cum2[b], 3) + [zero8], axis=0).astype(BF16), pick_own)
        dt_cols = dot_tt(jnp.concatenate(split(dts[b], 2), axis=0).astype(BF16), spread[:, WIDE:])
        xb = xv[rows, :]
        same = jnp.sum(c_b.astype(F32) * b_b.astype(F32), axis=1, keepdims=True)
        rest = xb.astype(F32) * (same * dt_cols + skip_row)
        for pair in range(2):
            halves = []
            for h in (2 * pair, 2 * pair + 1):
                gaps = jnp.where(
                    after,
                    cols[:, h : h + 1] - cprime[b][h : h + 1, :],
                    cols[:, 4 + h : 5 + h] - cprime[b][4 + h : 5 + h, :],
                )
                weights = (scores * jnp.exp2(gaps)).astype(BF16)
                halves.append(dot(weights, xb[:, pair * 128 : (pair + 1) * 128]))
            lanes = slice(pair * 128, (pair + 1) * 128)
            yv[b, :, lanes] = jnp.where(lane < 64, halves[0], halves[1]) + rest[:, lanes]

    def enter():
        phase("carry")
        arrived(carry, st_send.at[0], st_recv.at[0], other)
        came = carry[...]
        nothing = jnp.zeros_like(came)
        state = jnp.where(seq == 1, came, nothing)
        for b in range(BLOCKS):
            ef[b] = state.astype(BF16)
            state = decays[b][0] * state + sf[b]
        state = jnp.where(seq == 0, came, nothing)
        for b in reversed(range(BLOCKS)):
            eb[b] = state.astype(BF16)
            state = decays[b][1] * state + sb[b]
        loads[6].wait()
        loads[8].wait()
        ss1[my_y] = jnp.zeros((8, 128), F32)
        ss2[my_x] = jnp.zeros((8, 128), F32)

    ones8 = jnp.ones((8, WIDE), BF16)

    def gate(b):
        phase(f"gate{b}")
        rows = slice(b * SPAN, (b + 1) * SPAN)
        e_cols = dot_tt(jnp.concatenate(split(grows[b], 2), axis=0).astype(BF16), spread)
        inter_f = dot(pfv[1, rows, :], ef[b]) * e_cols[:, :WIDE]
        inter_b = dot(pbv[1, rows, :], eb[b]) * e_cols[:, WIDE:]
        zb = zv[rows, :].astype(F32)
        gated = (yv[b] + inter_f + inter_b) * (zb / (1.0 + jnp.exp(-zb)))
        g = (gated * gain_ref[...]).astype(BF16)
        a1[my_y, b] = g[:HALF]
        a2[my_x, b] = g[HALF:]
        square = split(gated * gated, 2)
        sums = dot_nt(ones8, square[0].astype(BF16)) + dot_nt(ones8, square[1].astype(BF16))
        ss1[my_y, b : b + 1, :] = sums[0:1, :HALF]
        ss2[my_x, b : b + 1, :] = sums[0:1, HALF:]
        if b == BLOCKS - 1:
            for k in (1, 0, 2):
                for p, plan in enumerate(plans):
                    ss, mine, dev = plan[4], plan[6], plan[8]
                    start(ss.at[mine], ss.at[mine], s_send.at[p], s_recv.at[p], dev[k])
        for k in (0, 2):
            for p, plan in enumerate(plans):
                a, mine, dev = plan[0], plan[6], plan[8]
                start(a.at[mine, b], a.at[mine, b], a_send.at[p], a_recv.at[p, b], dev[k])

    def send_far(b):
        phase(f"far{b}")
        for p, plan in enumerate(plans):
            a, mine, dev = plan[0], plan[6], plan[8]
            start(a.at[mine, b], a.at[mine, b], a_send.at[p], a_recv.at[p, b], dev[1])

    def relay(b):
        phase(f"relay{b}")
        for p, plan in enumerate(plans):
            a, src, dev = plan[0], plan[7], plan[8]
            arrived(a.at[pl.ds(0, 2), b], a_send.at[p], a_recv.at[p, b], dev[0])
            for i, k in enumerate((2, 0)):
                half = a.at[src[k], b, pl.ds(i * 64, 64)]
                start(half, half, a_send.at[p], r_recv.at[p, b], dev[2 - k])

    def product(b):
        for p, (a, w, o, dest, ss, so, _, _, dev, mine, peers, back) in enumerate(plans):
            phase(f"wait{b}{p}")
            if b in RELAYED:
                arrived(a.at[0, b], a_send.at[p], r_recv.at[p, b], dev[0])
            else:
                arrived(a.at[pl.ds(0, 3), b], a_send.at[p], a_recv.at[p, b], dev[0])
            phase(f"product{b}{p}")
            lhs = jnp.concatenate([a[j, b] for j in range(SIDE)], axis=1)
            values = dot(lhs, w[...].reshape(SIDE * WIDE, SIDE * COLS)).astype(BF16)
            for j in range(SIDE):
                o[b, j] = values[:, j * COLS : (j + 1) * COLS]
            for k in (1, 0, 2):
                start(o.at[b, peers[k]], dest.at[mine, b], o_send.at[p], o_recv.at[p, b], back[k])

    def squares():
        phase("squares")
        for p, (_, _, _, _, ss, so, _, _, dev, mine, _, back) in enumerate(plans):
            arrived(ss.at[pl.ds(0, 3)], s_send.at[p], s_recv.at[p], dev[0])
            so[mine] = ss[0] + ss[1] + ss[2] + ss[3]
            for k in (1, 0, 2):
                start(so.at[mine], so.at[mine], t_send.at[p], t_recv.at[p], back[k])

    intra(0)
    enter()
    gate(0)
    intra(1)
    gate(1)
    intra(2)
    gate(2)
    pass_weights_on()
    intra(3)
    gate(3)
    relay(0)
    relay(1)
    all_weights()
    relay(2)
    send_far(3)
    product(0)
    squares()
    product(1)
    product(2)
    product(3)

    phase("scale")
    scales = []
    for p, plan in enumerate(plans):
        so, back = plan[5], plan[11]
        arrived(so.at[pl.ds(0, 3)], t_send.at[p], t_recv.at[p], back[0])
        scale = lax.rsqrt((so[0] + so[1] + so[2] + so[3]) / INNER + 1.0)
        parts = split(scale, 3) + [jnp.zeros((8, 128), F32)]
        scales.append(jnp.concatenate(parts, axis=0).astype(BF16))
    for b in range(BLOCKS):
        phase(f"out{b}")
        pick_b = pick(b)
        for p, (_, _, o, dest, _, _, _, _, _, mine, peers, back) in enumerate(plans):
            scale = dot_tt(scales[p], pick_b)
            arrived(dest.at[pl.ds(0, 3), b], o_send.at[p], o_recv.at[p, b], back[0])
            total = o[b, mine].astype(F32)
            for k in range(3):
                total = total + dest[peers[k], b].astype(F32)
            at = b * SPAN + p * HALF
            out_ref[at : at + HALF, :] = (total * scale).astype(BF16)

    phase("drain")
    remote(payload, carry, st_send.at[0], st_recv.at[0], other).wait_send()
    for p, (a, w, o, dest, ss, so, _, _, dev, _, _, back) in enumerate(plans):
        for ref, send, recv in (
            (three(w), w_send.at[p], w_recv.at[p]),
            (three(w), v_send.at[p], v_recv.at[p]),
            (a.at[pl.ds(0, 3)], a_send.at[p], a_recv.at[p, 0]),
            (ss.at[pl.ds(0, 3)], s_send.at[p], s_recv.at[p]),
            (so.at[pl.ds(0, 3)], t_send.at[p], t_recv.at[p]),
            (o.at[:, pl.ds(0, 3)], o_send.at[p], o_recv.at[p, 0]),
        ):
            remote(ref, ref, send, recv, dev[0]).wait_send()
    phase(None)


def body(ssm_input, gate_z, proj_forward, proj_backward, step_raw, head_params, skip_gain, norm_gain, out_weight):
    hbm = pl.BlockSpec(memory_space=pltpu.HBM)
    dma = pltpu.SemaphoreType.DMA
    rows = BLOCKS * SPAN
    return pl.pallas_call(
        kernel,
        out_shape=jax.ShapeDtypeStruct((rows, COLS), BF16),
        in_specs=[hbm] * 9,
        out_specs=pl.BlockSpec(memory_space=pltpu.VMEM),
        scratch_shapes=[
            pltpu.VMEM((SIDE, SIDE, WIDE, COLS), BF16),
            pltpu.SMEM((2, 2, HEADS), F32),
            pltpu.SMEM((HEADS,), F32),
            pltpu.VMEM((1, WIDE), F32),
            pltpu.VMEM((rows, WIDE), BF16),
            pltpu.VMEM((rows, WIDE), BF16),
            pltpu.VMEM((2, rows, NST), BF16),
            pltpu.VMEM((2, rows, NST), BF16),
            pltpu.VMEM((2, HEADS, rows), F32),
            *[pltpu.VMEM((SIDE, WIDE, SIDE * COLS), BF16)] * 2,
            *[pltpu.VMEM((SIDE, BLOCKS, HALF, WIDE), BF16)] * 2,
            *[pltpu.VMEM((BLOCKS, SIDE, HALF, COLS), BF16)] * 2,
            *[pltpu.VMEM((SIDE, BLOCKS, HALF, COLS), BF16)] * 2,
            *[pltpu.VMEM((SIDE, 8, 128), F32)] * 4,
            pltpu.VMEM((BLOCKS, SPAN, WIDE), F32),
            *[pltpu.VMEM((BLOCKS, NST, WIDE), F32)] * 2,
            *[pltpu.VMEM((BLOCKS, NST, WIDE), BF16)] * 2,
            *[pltpu.VMEM((NST, WIDE), F32)] * 2,
            dma((11,)),
            *[dma((2,))] * 4,
            *[dma((1,))] * 2,
            dma((2,)),
            dma((2, BLOCKS)),
            dma((2, BLOCKS - 1)),
            *[dma((2,))] * 5,
            dma((2, BLOCKS)),
        ],
        compiler_params=pltpu.CompilerParams(
            collective_id=0, has_side_effects=True, vmem_limit_bytes=48 * 1024 * 1024
        ),
        name="encoder",
    )(*[
        pltpu.with_memory_space_constraint(v, pltpu.HBM)
        for v in (
            ssm_input, gate_z, proj_forward, proj_backward, step_raw, head_params, skip_gain,
            norm_gain.reshape(1, WIDE), out_weight.reshape(SIDE, SIDE, WIDE, COLS),
        )
    ])


def solution(mesh):
    in_specs = (
        P(("batch", "seq"), "chan"),
        P(("batch", "seq"), "chan"),
        P(None, ("batch", "seq"), None),
        P(None, ("batch", "seq"), None),
        P(None, "chan", ("batch", "seq")),
        P(None, None, "chan"),
        P("chan"),
        P("chan"),
        P(None, "chan"),
    )
    out_specs = P(("batch", "seq"), "chan")
    return jax.shard_map(body, mesh=mesh, in_specs=in_specs, out_specs=out_specs, check_vma=False)
```
